32 devices in a mesh: slab: 4 (over x, core), rep: 8 (over z, y).
Axes of the slice: x: 2, y: 2, z: 4, core: 2. Of those that a mesh axis runs over, the one named last changes fastest.
Arguments:
- image: float32 [144, 256, 256], P('slab', 'rep'), may hold values from 0.5 to 2
- sensitivity: float32 [144, 256, 256], P('slab', 'rep'), may hold values from 0.5 to 2
- system_blocks: bfloat16 [512, 128, 1024], P(('slab', 'rep')), may hold values from 0 to 0.00390625
- tile_slab: int32 [512, 1], P(('slab', 'rep')), may hold values from 0 to 3; in each aligned block of 16 rows (0 to 15, 16 to 31, ...) at most 6 rows name the same one
- tile_block: int32 [512], P(('slab', 'rep')), may hold values from 0 to 2303
- background: bfloat16 [512, 128], P(('slab', 'rep')), may hold values from 0.19921875 to 1
Outputs:
- updated: float32 [144, 256, 256], P('slab', 'rep')
The draws below stay inside these ranges and needn't reach their ends.
Inputs may be any that keep to these rules, and one draw needn't show every extreme that they name: `tile_slab`: among the 16 tiles of one device at most 6 view the same slab, and in some devices some slab is viewed by exactly 6.
All inputs are finite; a program needn't handle non-finite values.
Results may differ from the reference program's by a relative error of at most 0.0003.
Values may be sent and summed in bfloat16 or wider, within the bound.
A program may use at most 64 MiB of HBM per device.

```python
import math
import jax
import jax.numpy as jnp
import numpy as np
from jax import lax

NX = 256
NY = 256
TILE = 128
VB = 1024
PIECES_PER_CARD = 16
CAP = 6
NZ = 144
NBLK = 2304
TILES = 512
N_SLAB = 4


def place_ends(entries, own_key, smallest, largest):
    dims = entries.shape
    place = [jax.random.randint(jax.random.fold_in(own_key, axis), (), 0, dims[axis]) for axis in range(len(dims))]
    entries = entries.at[tuple(place)].set(smallest)
    longest = dims.index(max(dims))
    place[longest] = (place[longest] + 1) % dims[longest]
    return entries.at[tuple(place)].set(largest)


def level_of(rng, dims, pieces, low, top_value):
    def one(axis_at, blocks):
        draws = jax.random.uniform(jax.random.fold_in(jax.random.fold_in(rng, 6), axis_at), (blocks,), jnp.float32, low / len(pieces), top_value / len(pieces))
        return jnp.repeat(jnp.exp(draws), dims[axis_at] // blocks).reshape((-1,) + (1,) * (len(dims) - axis_at - 1))

    level = one(*pieces[0])
    for cut in pieces[1:]:
        level = level * one(*cut)
    return level


def assign_block(key, own, number, rows, amount, top, limit, skew):
    ranking = jax.random.permutation(key, amount)
    heavy_load, ordinary = portions_of(amount, rows * top, limit, skew, True), portions_of(amount, rows * top, limit, skew, False)
    places = jnp.arange(amount)

    def named(sizes, turn):
        used = int((sizes > 0).sum())
        fixed = max(1, used // 4)
        shifted = fixed + (places - fixed + turn * (used - fixed)) % max(1, amount - fixed)
        return jnp.zeros((amount,), jnp.int32).at[ranking[jnp.where(places < fixed, places, shifted)]].set(jnp.asarray(sizes, jnp.int32))

    sizes = jnp.where(number % 4 == 0, named(heavy_load, number // 4), named(ordinary, number - number // 4 - 1))
    mixed = jax.random.permutation(jax.random.fold_in(own, 3), amount)
    giver, sink = mixed[0:amount // 2 * 2:2], mixed[1:amount // 2 * 2:2]
    margin = jnp.minimum(sizes[giver] - 1, limit - sizes[sink]) // 2
    margin = jnp.where((giver == ranking[0]) | (sink == ranking[0]) | (sizes[sink] == 0), 0, jnp.maximum(margin, 0))
    shifted = jax.random.randint(jax.random.fold_in(own, 4), (amount // 2,), 0, 1 << 20) % (margin + 1)
    sizes = sizes.at[giver].add(-shifted).at[sink].add(shifted)
    labels = jnp.searchsorted(jnp.cumsum(sizes), jnp.arange(rows * top), side="right").astype(jnp.int32)
    listing = labels.reshape(top, rows).T
    listing = listing[jax.random.permutation(jax.random.fold_in(own, 1), rows)]
    turn = jax.random.randint(jax.random.fold_in(own, 2), (rows, 1), 0, top)
    return jnp.take_along_axis(listing, (jnp.arange(top)[None, :] + turn) % top, axis=1)


def portions_of(count, total, reach, skew, full):
    portions = [(1 << 20) // math.isqrt(standing ** skew) + 1 for standing in range(1, count + 1)]
    largest = reach if full else min(reach, max(-(-total // count), total * portions[0] // sum(portions)))
    least = 1 if total - largest >= count - 1 else 0
    given, surplus = [largest] + [least] * (count - 1), total - largest - least * (count - 1)
    while surplus > 0:
        free = [i for i in range(1, count) if given[i] < largest] or [i for i in range(1, count) if given[i] < reach]
        whole, remaining = sum([portions[i] for i in free]), surplus
        for i in free:
            more = min(reach - given[i], max(1, remaining * portions[i] // whole), surplus)
            given[i] = given[i] + more
            surplus = surplus - more
    return np.array(given)


def setup_inputs(seed: int = 0) -> dict:
    splits = jax.random.split(jax.random.key(seed), 7)
    image = jnp.clip(jnp.exp(math.log(2.0) - 1.3862944 * jax.random.uniform(splits[0], (NZ, NY, NX), jnp.float32) ** level_of(splits[0], (NZ, NY, NX), ((0, 4), (1, 8)), -0.2, 0.2)), 0.5, 2.0)
    sensitivity = jnp.clip(jnp.exp(math.log(2.0) - 1.3862944 * jax.random.uniform(splits[1], (NZ, NY, NX), jnp.float32) ** level_of(splits[1], (NZ, NY, NX), ((0, 4), (1, 8)), -0.2, 0.2)), 0.5, 2.0)
    system_blocks = jnp.clip(0.00390625 * jax.random.uniform(splits[2], (TILES, TILE, VB), jnp.float32) ** level_of(splits[2], (TILES, TILE, VB), ((0, 32),), -0.2, 0.2), 0.0, 0.00390625).astype(jnp.bfloat16)
    tile_slab_keys = jax.random.split(jax.random.fold_in(splits[3], 1), TILES // PIECES_PER_CARD)
    tile_slab_turns = jax.random.permutation(jax.random.fold_in(splits[3], 3), TILES // PIECES_PER_CARD)
    tile_slab = jax.vmap(lambda own, number: assign_block(jax.random.fold_in(splits[3], 2), own, number, PIECES_PER_CARD, N_SLAB, 1, CAP, 2))(tile_slab_keys, tile_slab_turns).reshape((TILES, 1))
    tile_block = place_ends(jax.random.randint(splits[4], (TILES,), 0, NBLK), jax.random.fold_in(splits[4], 1), 0, NBLK - 1).astype(jnp.int32)
    background = jnp.clip(jnp.exp(math.log(1.0) - 1.6133518 * jax.random.uniform(splits[5], (TILES, TILE), jnp.float32) ** level_of(splits[5], (TILES, TILE), ((0, 32),), -0.2, 0.2)), 0.19921875, 1.0).astype(jnp.bfloat16)
    return dict(image=image, sensitivity=sensitivity, system_blocks=system_blocks, tile_slab=tile_slab, tile_block=tile_block, background=background)


def reference(image, sensitivity, system_blocks, tile_slab, tile_block, background):
    tile_rows = system_blocks.shape[1]
    width = system_blocks.shape[2]
    unrolled_emission_map = image.astype(jnp.bfloat16).reshape(-1, width)
    index = (tile_slab[:, 0].astype(jnp.int32) * NBLK + tile_block.astype(jnp.int32)).astype(jnp.int32)

    def one_group(group):
        response_operator_lines, rows_index, back_ground = group
        emission_cell_entries = unrolled_emission_map[rows_index].astype(jnp.float32)
        sys_wide = response_operator_lines.astype(jnp.float32)
        forward_projection = jnp.einsum('tev,tv->te', sys_wide, emission_cell_entries, precision=lax.Precision.HIGHEST)
        inverse_permutation = (1.0 / (forward_projection + back_ground.astype(jnp.float32))).astype(jnp.bfloat16)
        inverse_permutation = lax.optimization_barrier(inverse_permutation)
        return jnp.einsum('tev,te->tv', sys_wide, inverse_permutation.astype(jnp.float32), precision=lax.Precision.HIGHEST)

    groups = (system_blocks.reshape(-1, 16, tile_rows, width), index.reshape(-1, 16), background.reshape(-1, 16, tile_rows))
    backproj = lax.map(one_group, groups).reshape(-1, width)
    partial_value = jnp.zeros(unrolled_emission_map.shape, jnp.float32).at[index].add(backproj)
    return image * partial_value.reshape(image.shape) / sensitivity
```

```python
import functools

import jax
import jax.numpy as jnp
from jax import lax
from jax.experimental import pallas as pl
from jax.experimental.pallas import tpu as pltpu
from jax.sharding import PartitionSpec as P

CAP = 6
LANES = 128
MESH = pl.DeviceIdType.MESH


def exchange_kernel(
    sizes, meta_ref, image_hbm, sys_hbm, bg_ref, asked_ref, back_ref,
    image_v, blocks_v, sys_v, mine_v, slot_v, mine_s, slot_s, asked_s, send_f, recv_f, bp_v, send_b,
    local_sem, id_sem, fetch_sem, back_sem,
):
    n, reps, tiles, block_rows = sizes
    me = lax.axis_index("slab") * reps + lax.axis_index("rep")
    lane_tiles = image_v.shape[1] // LANES

    def device(d):
        return (d // reps, d % reps)

    load_sys = pltpu.make_async_copy(sys_hbm, sys_v, local_sem.at[0])
    load_image = pltpu.make_async_copy(image_hbm, image_v, local_sem.at[1])
    load_image.start()
    load_sys.start()

    barrier = pltpu.get_barrier_semaphore()

    def greet(i, c):
        pl.semaphore_signal(barrier, inc=1, device_id=device((me + i) % n), device_id_type=MESH)
        return c

    lax.fori_loop(1, n, greet, 0)

    key = meta_ref[0:1, :]
    value = meta_ref[1:2, :]
    hot = key == lax.broadcasted_iota(jnp.int32, (n, LANES), 0)
    earlier = lax.broadcasted_iota(jnp.int32, (LANES, LANES), 0) < lax.broadcasted_iota(
        jnp.int32, (LANES, LANES), 1
    )
    rank = jnp.dot(
        jnp.where(hot, 1.0, 0.0).astype(jnp.bfloat16),
        jnp.where(earlier, 1.0, 0.0).astype(jnp.bfloat16),
        preferred_element_type=jnp.float32,
    ).astype(jnp.int32)
    lane = lax.broadcasted_iota(jnp.int32, (n, LANES), 1)
    table = jnp.zeros((n, LANES), jnp.int32)
    for k in range(CAP):
        picked = jnp.sum(jnp.where(hot & (rank == k), value, 0), axis=1, keepdims=True)
        table = jnp.where(lane == k, picked, table)
    mine_v[...] = table
    own_rank = jnp.sum(jnp.where(hot, rank, 0), axis=0, keepdims=True)
    away = key - me
    slot = jnp.where(away < 0, away + n, away) * CAP + own_rank
    slot_v[...] = jnp.broadcast_to(jnp.clip(slot, 0, n * CAP - 1), slot_v.shape)
    to_slot = pltpu.make_async_copy(slot_v, slot_s, local_sem.at[2])
    to_slot.start()
    to_mine = pltpu.make_async_copy(mine_v, mine_s, local_sem.at[3])
    to_mine.start()
    asked_ref[pl.ds(0, 1), :] = mine_v[pl.ds(me, 1), :]

    pl.semaphore_wait(barrier, n - 1)

    def id_copy(i):
        d = (me + i) % n
        return pltpu.make_async_remote_copy(
            src_ref=mine_v.at[pl.ds(d, 1)], dst_ref=asked_ref.at[pl.ds(i, 1)],
            send_sem=id_sem.at[0], recv_sem=id_sem.at[1],
            device_id=device(d), device_id_type=MESH,
        )

    def send_ids(i, c):
        id_copy(i).start()
        return c

    lax.fori_loop(1, n, send_ids, 0)
    to_slot.wait()
    to_mine.wait()
    load_image.wait()
    per_group = 8 // block_rows

    def cut(g, c):
        rows = image_v[pl.ds(pl.multiple_of(g * 8, 8), 8), :].astype(jnp.bfloat16).astype(jnp.float32)
        for u in range(per_group):
            blocks_v[g * per_group + u] = jnp.concatenate(
                [
                    rows[u * block_rows:(u + 1) * block_rows, h * LANES:(h + 1) * LANES]
                    for h in range(lane_tiles)
                ],
                axis=0,
            ).astype(jnp.bfloat16)
        return c

    lax.fori_loop(0, image_v.shape[0] // 8, cut, 0, unroll=4)
    rest = asked_ref.at[pl.ds(1, n - 1)]
    pltpu.make_async_copy(rest, rest, id_sem.at[1]).wait()
    to_asked = pltpu.make_async_copy(asked_ref, asked_s, local_sem.at[2])
    to_asked.start()
    to_asked.wait()

    def served(i, k):
        return blocks_v[jnp.maximum(asked_s[i, k] - 1, 0) // tiles]

    for k in range(CAP):
        recv_f[k] = served(0, k)

    def serve(i, c):
        for k in range(CAP):
            send_f[i * CAP + k] = served(i, k)
        span = pl.ds(i * CAP, CAP)
        pltpu.make_async_remote_copy(
            src_ref=send_f.at[span], dst_ref=recv_f.at[span],
            send_sem=fetch_sem.at[0], recv_sem=fetch_sem.at[1],
            device_id=device((me + n - i) % n), device_id_type=MESH,
        ).start()
        return c

    lax.fori_loop(1, n, serve, 0)
    background = jnp.transpose(bg_ref[...].astype(jnp.float32))
    load_sys.wait()
    others = recv_f.at[pl.ds(CAP, (n - 1) * CAP)]
    pltpu.make_async_copy(others, others, fetch_sem.at[1]).wait()

    for t in range(tiles):
        cells = recv_f[slot_s[0, t]].astype(jnp.float32)
        total = None
        for p in range(block_rows * lane_tiles):
            q = (p % block_rows) * lane_tiles + p // block_rows
            term = sys_v[t, :, q * LANES:(q + 1) * LANES].astype(jnp.float32) * cells[p:p + 1, :]
            total = term if total is None else total + term
        forward = jnp.sum(total, axis=1, keepdims=True)
        inverse = (1.0 / (forward + background[:, t:t + 1])).astype(jnp.bfloat16).astype(jnp.float32)
        parts = []
        for p in range(block_rows * lane_tiles):
            q = (p % block_rows) * lane_tiles + p // block_rows
            term = sys_v[t, :, q * LANES:(q + 1) * LANES].astype(jnp.float32) * inverse
            parts.append(jnp.sum(term, axis=0, keepdims=True))
        bp_v[t] = jnp.concatenate(parts, axis=0)

    def routed(d, k):
        return bp_v[jnp.maximum(mine_s[d, k] - 1, 0) % tiles]

    for k in range(CAP):
        back_ref[k] = routed(me, k)

    def give(i, c):
        d = (me + i) % n
        for k in range(CAP):
            send_b[i * CAP + k] = routed(d, k)
        span = pl.ds(i * CAP, CAP)
        pltpu.make_async_remote_copy(
            src_ref=send_b.at[span], dst_ref=back_ref.at[span],
            send_sem=back_sem.at[0], recv_sem=back_sem.at[1],
            device_id=device(d), device_id_type=MESH,
        ).start()
        return c

    lax.fori_loop(1, n, give, 0)
    pltpu.make_async_copy(mine_v.at[pl.ds(1, n - 1)], mine_v.at[pl.ds(1, n - 1)], id_sem.at[0]).wait()
    sent = send_f.at[pl.ds(CAP, (n - 1) * CAP)]
    pltpu.make_async_copy(sent, sent, fetch_sem.at[0]).wait()
    given = send_b.at[pl.ds(CAP, (n - 1) * CAP)]
    pltpu.make_async_copy(given, given, back_sem.at[0]).wait()
    landed = back_ref.at[pl.ds(CAP, (n - 1) * CAP)]
    pltpu.make_async_copy(landed, landed, back_sem.at[1]).wait()


def update_kernel(sizes, asked_s, back_ref, image_ref, sens_ref, out_ref, sums_v):
    n, tiles, block_rows = sizes
    lane_tiles = out_ref.shape[1] // LANES
    per_group = 8 // block_rows
    sums_v[...] = jnp.zeros_like(sums_v)

    def add(i, k):
        if k == CAP:
            return
        value = asked_s[i, k]

        @pl.when(value > 0)
        def _():
            sums_v[(value - 1) // tiles] += back_ref[i * CAP + k]
            add(i, k + 1)

    def one(i, c):
        add(i, 0)
        return c

    lax.fori_loop(0, n, one, 0)

    def finish(g, c):
        rows = pl.ds(pl.multiple_of(g * 8, 8), 8)
        sums = [sums_v[g * per_group + u] for u in range(per_group)]
        for h in range(lane_tiles):
            cols = slice(h * LANES, (h + 1) * LANES)
            total = jnp.concatenate([s[h * block_rows:(h + 1) * block_rows] for s in sums], axis=0)
            out_ref[rows, cols] = image_ref[rows, cols] * total / sens_ref[rows, cols]
        return c

    lax.fori_loop(0, out_ref.shape[0] // 8, finish, 0, unroll=4)


def local(image, sensitivity, system_blocks, tile_slab, tile_block, background):
    slabs, reps = lax.axis_size("slab"), lax.axis_size("rep")
    n = slabs * reps
    tiles, events, width = system_blocks.shape
    planes, rows, cols = image.shape
    block_rows = width // cols
    per_owner = rows // block_rows
    per_plane = per_owner * reps
    within = tile_block % per_plane
    key = tile_slab[:, 0] * reps + within // per_owner
    local_id = (tile_block // per_plane) * per_owner + within % per_owner
    value = local_id * tiles + jnp.arange(tiles, dtype=jnp.int32) + 1
    meta = jnp.full((8, LANES), -1, jnp.int32).at[0, :tiles].set(key).at[1, :tiles].set(value)
    image2 = image.reshape(planes * rows, cols)
    sens2 = sensitivity.reshape(planes * rows, cols)
    sub = width // LANES

    vmem = pl.BlockSpec(memory_space=pltpu.VMEM)
    hbm = pl.BlockSpec(memory_space=pl.ANY)
    asked, back = pl.pallas_call(
        functools.partial(exchange_kernel, (n, reps, tiles, block_rows)),
        out_shape=(
            jax.ShapeDtypeStruct((n, LANES), jnp.int32),
            jax.ShapeDtypeStruct((n * CAP, sub, LANES), jnp.float32),
        ),
        in_specs=[vmem, hbm, hbm, vmem],
        out_specs=(vmem, vmem),
        scratch_shapes=[
            pltpu.VMEM(image2.shape, jnp.float32),
            pltpu.VMEM((planes * per_owner, sub, LANES), jnp.bfloat16),
            pltpu.VMEM(system_blocks.shape, jnp.bfloat16),
            pltpu.VMEM((n, LANES), jnp.int32),
            pltpu.VMEM((8, LANES), jnp.int32),
            pltpu.SMEM((n, LANES), jnp.int32),
            pltpu.SMEM((8, LANES), jnp.int32),
            pltpu.SMEM((n, LANES), jnp.int32),
            pltpu.VMEM((n * CAP, sub, LANES), jnp.bfloat16),
            pltpu.VMEM((n * CAP, sub, LANES), jnp.bfloat16),
            pltpu.VMEM((tiles, sub, LANES), jnp.float32),
            pltpu.VMEM((n * CAP, sub, LANES), jnp.float32),
            pltpu.SemaphoreType.DMA((4,)),
            pltpu.SemaphoreType.DMA((2,)),
            pltpu.SemaphoreType.DMA((2,)),
            pltpu.SemaphoreType.DMA((2,)),
        ],
        compiler_params=pltpu.CompilerParams(
            collective_id=0, has_side_effects=True, vmem_limit_bytes=48 * 1024 * 1024
        ),
    )(meta, image2, system_blocks, background)
    updated = pl.pallas_call(
        functools.partial(update_kernel, (n, tiles, block_rows)),
        out_shape=jax.ShapeDtypeStruct(image2.shape, jnp.float32),
        in_specs=[pl.BlockSpec(memory_space=pltpu.SMEM), vmem, vmem, vmem],
        out_specs=vmem,
        scratch_shapes=[pltpu.VMEM((planes * per_owner, sub, LANES), jnp.float32)],
        compiler_params=pltpu.CompilerParams(vmem_limit_bytes=48 * 1024 * 1024),
    )(asked, back, image2, sens2)
    return updated.reshape(image.shape)


def solution(mesh):
    return jax.shard_map(
        local,
        mesh=mesh,
        in_specs=(
            P("slab", "rep", None),
            P("slab", "rep", None),
            P(("slab", "rep"), None, None),
            P(("slab", "rep"), None),
            P(("slab", "rep")),
            P(("slab", "rep"), None),
        ),
        out_specs=P("slab", "rep", None),
        check_vma=False,
    )
```

```python
import functools

import jax
import jax.numpy as jnp
from jax import lax
from jax.experimental import pallas as pl
from jax.experimental.pallas import tpu as pltpu
from jax.sharding import PartitionSpec as P

CAP = 6
LEVELS = 65535.0
HALF = 32768
LANES = 128
MESH = pl.DeviceIdType.MESH


def split(x, size):
    if size & (size - 1):
        return x // size, x % size
    return x >> (size.bit_length() - 1), x & (size - 1)


def exchange_kernel(
    sizes, slab_hbm, block_hbm, image_hbm, sys_hbm, bg_hbm, asked_ref, scale_ref, back_ref,
    slab_v, block_v, bg_v, scale_v, image_v, blocks_v, sys_v, mine_v, slot_v, mine_s, slot_s, asked_s, send_f, recv_f, bp_v, send_b,
    local_sem, id_sem, fetch_sem, back_sem, scale_sem,
):
    n, reps, tiles, block_rows, per_owner = sizes
    me = lax.axis_index("slab") * reps + lax.axis_index("rep")
    lane_tiles = image_v.shape[1] // LANES

    def device(d):
        return (d // reps, d % reps)

    load_sys = pltpu.make_async_copy(sys_hbm, sys_v, local_sem.at[0])
    load_image = pltpu.make_async_copy(image_hbm, image_v, local_sem.at[1])
    load_slab = pltpu.make_async_copy(slab_hbm, slab_v, local_sem.at[4])
    load_block = pltpu.make_async_copy(block_hbm, block_v, local_sem.at[5])
    load_bg = pltpu.make_async_copy(bg_hbm, bg_v, local_sem.at[6])
    for load in (load_slab, load_block, load_image, load_bg, load_sys):
        load.start()

    barrier = pltpu.get_barrier_semaphore()

    def greet(i, c):
        pl.semaphore_signal(barrier, inc=1, device_id=device((me + i) % n), device_id_type=MESH)
        return c

    lax.fori_loop(1, n, greet, 0)

    load_slab.wait()
    load_block.wait()
    block = block_v[...]
    plane, within = split(block, per_owner * reps)
    owner, offset = split(within, per_owner)
    key = slab_v[...] * reps + owner
    value = (plane * per_owner + offset) * tiles + lax.broadcasted_iota(jnp.int32, (1, tiles), 1) + 1
    hot = key == lax.broadcasted_iota(jnp.int32, (n, tiles), 0)
    square = (tiles, tiles)
    earlier = lax.broadcasted_iota(jnp.int32, square, 0) < lax.broadcasted_iota(jnp.int32, square, 1)
    rank = jnp.dot(
        jnp.where(hot, 1.0, 0.0).astype(jnp.bfloat16),
        jnp.where(earlier, 1.0, 0.0).astype(jnp.bfloat16),
        preferred_element_type=jnp.float32,
    ).astype(jnp.int32)
    lane = lax.broadcasted_iota(jnp.int32, (n, LANES), 1)

    def tabled(row, zero):
        table = jnp.full((n, LANES), zero)
        for k in range(CAP):
            picked = jnp.sum(jnp.where(hot & (rank == k), row, zero), axis=1, keepdims=True)
            table = jnp.where(lane == k, picked, table)
        return table

    mine_v[...] = tabled(value, jnp.int32(0))
    own_rank = jnp.sum(jnp.where(hot, rank, 0), axis=0, keepdims=True)
    away = key - me
    slot = jnp.where(away < 0, away + n, away) * CAP + own_rank
    slot_v[0:1, 0:tiles] = jnp.clip(slot, 0, n * CAP - 1)
    to_slot = pltpu.make_async_copy(slot_v, slot_s, local_sem.at[2])
    to_slot.start()
    to_mine = pltpu.make_async_copy(mine_v, mine_s, local_sem.at[3])
    to_mine.start()
    asked_ref[pl.ds(0, 1), :] = mine_v[pl.ds(me, 1), :]

    pl.semaphore_wait(barrier, n - 1)

    def id_copy(i):
        d = (me + i) % n
        return pltpu.make_async_remote_copy(
            src_ref=mine_v.at[pl.ds(d, 1)], dst_ref=asked_ref.at[pl.ds(i, 1)],
            send_sem=id_sem.at[0], recv_sem=id_sem.at[1],
            device_id=device(d), device_id_type=MESH,
        )

    def send_ids(i, c):
        id_copy(i).start()
        return c

    lax.fori_loop(1, n, send_ids, 0)
    to_slot.wait()
    to_mine.wait()
    load_image.wait()
    per_group = 8 // block_rows

    def cut(g, c):
        rows = image_v[pl.ds(pl.multiple_of(g * 8, 8), 8), :].astype(jnp.bfloat16).astype(jnp.float32)
        for u in range(per_group):
            blocks_v[g * per_group + u] = jnp.concatenate(
                [
                    rows[u * block_rows:(u + 1) * block_rows, h * LANES:(h + 1) * LANES]
                    for h in range(lane_tiles)
                ],
                axis=0,
            ).astype(jnp.bfloat16)
        return c

    lax.fori_loop(0, image_v.shape[0] // 8, cut, 0, unroll=4)
    rest = asked_ref.at[pl.ds(1, n - 1)]
    pltpu.make_async_copy(rest, rest, id_sem.at[1]).wait()
    to_asked = pltpu.make_async_copy(asked_ref, asked_s, local_sem.at[2])
    to_asked.start()
    to_asked.wait()

    def served(i, k):
        return blocks_v[jnp.maximum(asked_s[i, k] - 1, 0) // tiles]

    for k in range(CAP):
        recv_f[k] = served(0, k)

    def serve(i, c):
        for k in range(CAP):
            send_f[i * CAP + k] = served(i, k)
        span = pl.ds(i * CAP, CAP)
        pltpu.make_async_remote_copy(
            src_ref=send_f.at[span], dst_ref=recv_f.at[span],
            send_sem=fetch_sem.at[0], recv_sem=fetch_sem.at[1],
            device_id=device((me + n - i) % n), device_id_type=MESH,
        ).start()
        return c

    lax.fori_loop(1, n, serve, 0)
    load_bg.wait()
    background = jnp.transpose(bg_v[...].astype(jnp.float32))
    load_sys.wait()
    others = recv_f.at[pl.ds(CAP, (n - 1) * CAP)]
    pltpu.make_async_copy(others, others, fetch_sem.at[1]).wait()

    peaks = jnp.zeros((1, tiles), jnp.float32)
    tile_lane = lax.broadcasted_iota(jnp.int32, (1, tiles), 1)
    for t in range(tiles):
        cells = recv_f[slot_s[0, t]].astype(jnp.float32)
        total = None
        for p in range(block_rows * lane_tiles):
            q = (p % block_rows) * lane_tiles + p // block_rows
            term = sys_v[t, :, q * LANES:(q + 1) * LANES].astype(jnp.float32) * cells[p:p + 1, :]
            total = term if total is None else total + term
        forward = jnp.sum(total, axis=1, keepdims=True)
        inverse = (1.0 / (forward + background[:, t:t + 1])).astype(jnp.bfloat16).astype(jnp.float32)
        parts = []
        for p in range(block_rows * lane_tiles):
            q = (p % block_rows) * lane_tiles + p // block_rows
            term = sys_v[t, :, q * LANES:(q + 1) * LANES].astype(jnp.float32) * inverse
            parts.append(jnp.sum(term, axis=0, keepdims=True))
        tile = jnp.concatenate(parts, axis=0)
        peak = jnp.maximum(jnp.max(jnp.max(tile, axis=0, keepdims=True), axis=1, keepdims=True), 1e-33)
        level = jnp.round(tile * (LEVELS / peak)).astype(jnp.int32) - HALF
        bp_v[t] = jnp.clip(level, -HALF, HALF - 1).astype(jnp.int16)
        peaks = jnp.where(tile_lane == t, peak, peaks)
    scale_v[...] = tabled(peaks * (1.0 / LEVELS), jnp.float32(0))

    def routed(d, k):
        return bp_v[jnp.maximum(mine_s[d, k] - 1, 0) % tiles]

    for k in range(CAP):
        back_ref[k] = routed(me, k)

    def give(i, c):
        d = (me + i) % n
        for k in range(CAP):
            send_b[i * CAP + k] = routed(d, k)
        span = pl.ds(i * CAP, CAP)
        pltpu.make_async_remote_copy(
            src_ref=send_b.at[span], dst_ref=back_ref.at[span],
            send_sem=back_sem.at[0], recv_sem=back_sem.at[1],
            device_id=device(d), device_id_type=MESH,
        ).start()
        pltpu.make_async_remote_copy(
            src_ref=scale_v.at[pl.ds(d, 1)], dst_ref=scale_ref.at[pl.ds(i, 1)],
            send_sem=scale_sem.at[0], recv_sem=scale_sem.at[1],
            device_id=device(d), device_id_type=MESH,
        ).start()
        return c

    scale_ref[pl.ds(0, 1), :] = scale_v[pl.ds(me, 1), :]
    lax.fori_loop(1, n, give, 0)
    scaled = scale_ref.at[pl.ds(1, n - 1)]
    pltpu.make_async_copy(scaled, scaled, scale_sem.at[0]).wait()
    pltpu.make_async_copy(scaled, scaled, scale_sem.at[1]).wait()
    pltpu.make_async_copy(mine_v.at[pl.ds(1, n - 1)], mine_v.at[pl.ds(1, n - 1)], id_sem.at[0]).wait()
    sent = send_f.at[pl.ds(CAP, (n - 1) * CAP)]
    pltpu.make_async_copy(sent, sent, fetch_sem.at[0]).wait()
    given = send_b.at[pl.ds(CAP, (n - 1) * CAP)]
    pltpu.make_async_copy(given, given, back_sem.at[0]).wait()
    landed = back_ref.at[pl.ds(CAP, (n - 1) * CAP)]
    pltpu.make_async_copy(landed, landed, back_sem.at[1]).wait()


def update_kernel(sizes, asked_s, scale_s, back_ref, image_ref, sens_ref, out_ref, sums_v):
    n, tiles, block_rows = sizes
    lane_tiles = out_ref.shape[1] // LANES
    per_group = 8 // block_rows
    sums_v[...] = jnp.zeros_like(sums_v)

    def add(i, k):
        if k == CAP:
            return
        value = asked_s[i, k]

        @pl.when(value > 0)
        def _():
            level = back_ref[i * CAP + k].astype(jnp.int32) + HALF
            sums_v[(value - 1) // tiles] += level.astype(jnp.float32) * scale_s[i, k]
            add(i, k + 1)

    def one(i, c):
        add(i, 0)
        return c

    lax.fori_loop(0, n, one, 0)

    def finish(g, c):
        rows = pl.ds(pl.multiple_of(g * 8, 8), 8)
        sums = [sums_v[g * per_group + u] for u in range(per_group)]
        for h in range(lane_tiles):
            cols = slice(h * LANES, (h + 1) * LANES)
            total = jnp.concatenate([s[h * block_rows:(h + 1) * block_rows] for s in sums], axis=0)
            out_ref[rows, cols] = image_ref[rows, cols] * total / sens_ref[rows, cols]
        return c

    lax.fori_loop(0, out_ref.shape[0] // 8, finish, 0, unroll=4)


def local(image, sensitivity, system_blocks, tile_slab, tile_block, background):
    slabs, reps = lax.axis_size("slab"), lax.axis_size("rep")
    n = slabs * reps
    tiles, events, width = system_blocks.shape
    planes, rows, cols = image.shape
    block_rows = width // cols
    per_owner = rows // block_rows
    image2 = image.reshape(planes * rows, cols)
    sens2 = sensitivity.reshape(planes * rows, cols)
    sub = width // LANES

    vmem = pl.BlockSpec(memory_space=pltpu.VMEM)
    hbm = pl.BlockSpec(memory_space=pltpu.HBM)
    asked, scale, back = pl.pallas_call(
        functools.partial(exchange_kernel, (n, reps, tiles, block_rows, per_owner)),
        out_shape=(
            jax.ShapeDtypeStruct((n, LANES), jnp.int32),
            jax.ShapeDtypeStruct((n, LANES), jnp.float32),
            jax.ShapeDtypeStruct((n * CAP, sub, LANES), jnp.int16),
        ),
        in_specs=[hbm] * 5,
        out_specs=(vmem, vmem, vmem),
        scratch_shapes=[
            pltpu.VMEM((1, tiles), jnp.int32),
            pltpu.VMEM((1, tiles), jnp.int32),
            pltpu.VMEM(background.shape, jnp.bfloat16),
            pltpu.VMEM((n, LANES), jnp.float32),
            pltpu.VMEM(image2.shape, jnp.float32),
            pltpu.VMEM((planes * per_owner, sub, LANES), jnp.bfloat16),
            pltpu.VMEM(system_blocks.shape, jnp.bfloat16),
            pltpu.VMEM((n, LANES), jnp.int32),
            pltpu.VMEM((8, LANES), jnp.int32),
            pltpu.SMEM((n, LANES), jnp.int32),
            pltpu.SMEM((8, LANES), jnp.int32),
            pltpu.SMEM((n, LANES), jnp.int32),
            pltpu.VMEM((n * CAP, sub, LANES), jnp.bfloat16),
            pltpu.VMEM((n * CAP, sub, LANES), jnp.bfloat16),
            pltpu.VMEM((tiles, sub, LANES), jnp.int16),
            pltpu.VMEM((n * CAP, sub, LANES), jnp.int16),
            pltpu.SemaphoreType.DMA((7,)),
            pltpu.SemaphoreType.DMA((2,)),
            pltpu.SemaphoreType.DMA((2,)),
            pltpu.SemaphoreType.DMA((2,)),
            pltpu.SemaphoreType.DMA((2,)),
        ],
        compiler_params=pltpu.CompilerParams(
            collective_id=0, has_side_effects=True, vmem_limit_bytes=62914560
        ),
    )(tile_slab.reshape(1, tiles), tile_block.reshape(1, tiles), image2, system_blocks, background)
    updated = pl.pallas_call(
        functools.partial(update_kernel, (n, tiles, block_rows)),
        out_shape=jax.ShapeDtypeStruct(image2.shape, jnp.float32),
        in_specs=[pl.BlockSpec(memory_space=pltpu.SMEM)] * 2 + [vmem, vmem, vmem],
        out_specs=vmem,
        scratch_shapes=[pltpu.VMEM((planes * per_owner, sub, LANES), jnp.float32)],
        compiler_params=pltpu.CompilerParams(vmem_limit_bytes=48 * 1024 * 1024),
    )(asked, scale, back, image2, sens2)
    return updated.reshape(image.shape)


def solution(mesh):
    return jax.shard_map(
        local,
        mesh=mesh,
        in_specs=(
            P("slab", "rep", None),
            P("slab", "rep", None),
            P(("slab", "rep"), None, None),
            P(("slab", "rep"), None),
            P(("slab", "rep")),
            P(("slab", "rep"), None),
        ),
        out_specs=P("slab", "rep", None),
        check_vma=False,
    )
```

```python
import functools

import jax
import jax.numpy as jnp
from jax import lax
from jax.experimental import pallas as pl
from jax.experimental.pallas import tpu as pltpu
from jax.sharding import PartitionSpec as P

CAP = 6
LEVELS = 65535.0
HALF = 32768
LANES = 128
MESH = pl.DeviceIdType.MESH


def split(x, size):
    if size & (size - 1):
        return x // size, x % size
    return x >> (size.bit_length() - 1), x & (size - 1)


def exchange_kernel(
    sizes, slab_hbm, block_hbm, image_hbm, sys_hbm, bg_hbm, asked_ref, scale_ref, back_ref,
    slab_v, block_v, bg_v, scale_v, image_v, blocks_v, sys_v, mine_v, slot_v, mine_s, slot_s, asked_s, send_f, recv_f, sums_v, bp_v, send_b,
    local_sem, id_sem, fetch_sem, back_sem, scale_sem,
):
    n, reps, tiles, block_rows, per_owner = sizes
    me = lax.axis_index("slab") * reps + lax.axis_index("rep")
    lane_tiles = image_v.shape[1] // LANES

    def device(d):
        return (d // reps, d % reps)

    load_sys = pltpu.make_async_copy(sys_hbm, sys_v, local_sem.at[0])
    load_image = pltpu.make_async_copy(image_hbm, image_v, local_sem.at[1])
    load_slab = pltpu.make_async_copy(slab_hbm, slab_v, local_sem.at[4])
    load_block = pltpu.make_async_copy(block_hbm, block_v, local_sem.at[5])
    load_bg = pltpu.make_async_copy(bg_hbm, bg_v, local_sem.at[6])
    for load in (load_slab, load_block, load_image, load_bg, load_sys):
        load.start()

    barrier = pltpu.get_barrier_semaphore()

    def greet(i, c):
        pl.semaphore_signal(barrier, inc=1, device_id=device((me + i) % n), device_id_type=MESH)
        return c

    lax.fori_loop(1, n, greet, 0)

    load_slab.wait()
    load_block.wait()
    block = block_v[...]
    plane, within = split(block, per_owner * reps)
    owner, offset = split(within, per_owner)
    key = slab_v[...] * reps + owner
    value = (plane * per_owner + offset) * tiles + lax.broadcasted_iota(jnp.int32, (1, tiles), 1) + 1
    hot = key == lax.broadcasted_iota(jnp.int32, (n, tiles), 0)
    square = (tiles, tiles)
    earlier = lax.broadcasted_iota(jnp.int32, square, 0) < lax.broadcasted_iota(jnp.int32, square, 1)
    rank = jnp.dot(
        jnp.where(hot, 1.0, 0.0).astype(jnp.bfloat16),
        jnp.where(earlier, 1.0, 0.0).astype(jnp.bfloat16),
        preferred_element_type=jnp.float32,
    ).astype(jnp.int32)
    lane = lax.broadcasted_iota(jnp.int32, (n, LANES), 1)

    def tabled(row, zero):
        table = jnp.full((n, LANES), zero)
        for k in range(CAP):
            picked = jnp.sum(jnp.where(hot & (rank == k), row, zero), axis=1, keepdims=True)
            table = jnp.where(lane == k, picked, table)
        return table

    mine_v[...] = tabled(value, jnp.int32(0))
    own_rank = jnp.sum(jnp.where(hot, rank, 0), axis=0, keepdims=True)
    away = key - me
    slot = jnp.where(away < 0, away + n, away) * CAP + own_rank
    slot_v[0:1, 0:tiles] = jnp.clip(slot, 0, n * CAP - 1)
    to_slot = pltpu.make_async_copy(slot_v, slot_s, local_sem.at[2])
    to_slot.start()
    to_mine = pltpu.make_async_copy(mine_v, mine_s, local_sem.at[3])
    to_mine.start()
    asked_ref[pl.ds(0, 1), :] = mine_v[pl.ds(me, 1), :]

    pl.semaphore_wait(barrier, n - 1)

    def id_copy(i):
        d = (me + i) % n
        return pltpu.make_async_remote_copy(
            src_ref=mine_v.at[pl.ds(d, 1)], dst_ref=asked_ref.at[pl.ds(i, 1)],
            send_sem=id_sem.at[0], recv_sem=id_sem.at[1],
            device_id=device(d), device_id_type=MESH,
        )

    def send_ids(i, c):
        id_copy(i).start()
        return c

    lax.fori_loop(1, n, send_ids, 0)
    to_slot.wait()
    to_mine.wait()
    load_image.wait()
    per_group = 8 // block_rows

    def cut(g, c):
        rows = image_v[pl.ds(pl.multiple_of(g * 8, 8), 8), :].astype(jnp.bfloat16).astype(jnp.float32)
        for u in range(per_group):
            blocks_v[g * per_group + u] = jnp.concatenate(
                [
                    rows[u * block_rows:(u + 1) * block_rows, h * LANES:(h + 1) * LANES]
                    for h in range(lane_tiles)
                ],
                axis=0,
            ).astype(jnp.bfloat16)
        return c

    lax.fori_loop(0, image_v.shape[0] // 8, cut, 0, unroll=4)
    rest = asked_ref.at[pl.ds(1, n - 1)]
    pltpu.make_async_copy(rest, rest, id_sem.at[1]).wait()
    to_asked = pltpu.make_async_copy(asked_ref, asked_s, local_sem.at[2])
    to_asked.start()
    to_asked.wait()

    def served(i, k):
        return blocks_v[jnp.maximum(asked_s[i, k] - 1, 0) // tiles]

    for k in range(CAP):
        recv_f[k] = served(0, k)

    def serve(i, c):
        for k in range(CAP):
            send_f[i * CAP + k] = served(i, k)
        span = pl.ds(i * CAP, CAP)
        pltpu.make_async_remote_copy(
            src_ref=send_f.at[span], dst_ref=recv_f.at[span],
            send_sem=fetch_sem.at[0], recv_sem=fetch_sem.at[1],
            device_id=device((me + n - i) % n), device_id_type=MESH,
        ).start()
        return c

    lax.fori_loop(1, n, serve, 0)
    load_bg.wait()
    background = jnp.transpose(bg_v[...].astype(jnp.float32))
    load_sys.wait()
    others = recv_f.at[pl.ds(CAP, (n - 1) * CAP)]
    pltpu.make_async_copy(others, others, fetch_sem.at[1]).wait()

    forward = jnp.zeros(background.shape, jnp.float32)
    tile_lane = lax.broadcasted_iota(jnp.int32, (1, tiles), 1)
    pieces = block_rows * lane_tiles
    places = [(p % block_rows) * lane_tiles + p // block_rows for p in range(pieces)]
    for t in range(tiles):
        cells = recv_f[slot_s[0, t]].astype(jnp.float32)
        total = None
        for p, q in enumerate(places):
            term = sys_v[t, :, q * LANES:(q + 1) * LANES].astype(jnp.float32) * cells[p:p + 1, :]
            total = term if total is None else total + term
        forward = jnp.where(tile_lane == t, jnp.sum(total, axis=1, keepdims=True), forward)
    inverse = jnp.transpose(1.0 / (forward + background)).astype(jnp.bfloat16)
    tops = []
    for t in range(tiles):
        back = jnp.dot(inverse, sys_v[t], preferred_element_type=jnp.float32)
        tile = jnp.concatenate([back[t:t + 1, q * LANES:(q + 1) * LANES] for q in places], axis=0)
        sums_v[t] = tile
        tops.append(jnp.max(tile, axis=0, keepdims=True))
    peak = jnp.maximum(jnp.max(jnp.concatenate(tops, axis=0), axis=1, keepdims=True), 1e-33)
    gain = LEVELS / peak
    peaks = jnp.transpose(peak)
    for t in range(tiles):
        level = jnp.round(sums_v[t] * gain[t:t + 1, :]).astype(jnp.int32) - HALF
        bp_v[t] = jnp.clip(level, -HALF, HALF - 1).astype(jnp.int16)
    scale_v[...] = tabled(peaks * (1.0 / LEVELS), jnp.float32(0))

    def routed(d, k):
        return bp_v[jnp.maximum(mine_s[d, k] - 1, 0) % tiles]

    for k in range(CAP):
        back_ref[k] = routed(me, k)

    def give(i, c):
        d = (me + i) % n
        for k in range(CAP):
            send_b[i * CAP + k] = routed(d, k)
        span = pl.ds(i * CAP, CAP)
        pltpu.make_async_remote_copy(
            src_ref=send_b.at[span], dst_ref=back_ref.at[span],
            send_sem=back_sem.at[0], recv_sem=back_sem.at[1],
            device_id=device(d), device_id_type=MESH,
        ).start()
        pltpu.make_async_remote_copy(
            src_ref=scale_v.at[pl.ds(d, 1)], dst_ref=scale_ref.at[pl.ds(i, 1)],
            send_sem=scale_sem.at[0], recv_sem=scale_sem.at[1],
            device_id=device(d), device_id_type=MESH,
        ).start()
        return c

    scale_ref[pl.ds(0, 1), :] = scale_v[pl.ds(me, 1), :]
    lax.fori_loop(1, n, give, 0)
    scaled = scale_ref.at[pl.ds(1, n - 1)]
    pltpu.make_async_copy(scaled, scaled, scale_sem.at[0]).wait()
    pltpu.make_async_copy(scaled, scaled, scale_sem.at[1]).wait()
    pltpu.make_async_copy(mine_v.at[pl.ds(1, n - 1)], mine_v.at[pl.ds(1, n - 1)], id_sem.at[0]).wait()
    sent = send_f.at[pl.ds(CAP, (n - 1) * CAP)]
    pltpu.make_async_copy(sent, sent, fetch_sem.at[0]).wait()
    given = send_b.at[pl.ds(CAP, (n - 1) * CAP)]
    pltpu.make_async_copy(given, given, back_sem.at[0]).wait()
    landed = back_ref.at[pl.ds(CAP, (n - 1) * CAP)]
    pltpu.make_async_copy(landed, landed, back_sem.at[1]).wait()


def update_kernel(
    sizes, asked_hbm, scale_hbm, back_hbm, image_hbm, sens_hbm, out_hbm,
    asked_s, scale_s, back_ref, image_ref, sens_ref, out_ref, sums_v, in_sem, out_sem,
):
    n, tiles, block_rows = sizes
    moves = ((asked_hbm, asked_s), (scale_hbm, scale_s), (back_hbm, back_ref), (image_hbm, image_ref), (sens_hbm, sens_ref))
    loads = [pltpu.make_async_copy(src, dst, in_sem.at[j]) for j, (src, dst) in enumerate(moves)]
    for load in loads:
        load.start()
    lane_tiles = out_ref.shape[1] // LANES
    per_group = 8 // block_rows
    sums_v[...] = jnp.zeros_like(sums_v)

    def add(i, k):
        if k == CAP:
            return
        value = asked_s[i, k]

        @pl.when(value > 0)
        def _():
            level = back_ref[i * CAP + k].astype(jnp.int32) + HALF
            sums_v[(value - 1) // tiles] += level.astype(jnp.float32) * scale_s[i, k]
            add(i, k + 1)

    def one(i, c):
        add(i, 0)
        return c

    for load in loads[:3]:
        load.wait()
    lax.fori_loop(0, n, one, 0)
    for load in loads[3:]:
        load.wait()

    def finish(g, c):
        rows = pl.ds(pl.multiple_of(g * 8, 8), 8)
        sums = [sums_v[g * per_group + u] for u in range(per_group)]
        for h in range(lane_tiles):
            cols = slice(h * LANES, (h + 1) * LANES)
            total = jnp.concatenate([s[h * block_rows:(h + 1) * block_rows] for s in sums], axis=0)
            out_ref[rows, cols] = image_ref[rows, cols] * total / sens_ref[rows, cols]
        return c

    groups = out_ref.shape[0] // 8
    chunks = out_sem.shape[0]
    stores = []
    for c in range(chunks):
        first, last = groups * c // chunks, groups * (c + 1) // chunks
        lax.fori_loop(first, last, finish, 0, unroll=4)
        span = pl.ds(first * 8, (last - first) * 8)
        stores.append(pltpu.make_async_copy(out_ref.at[span], out_hbm.at[span], out_sem.at[c]))
        stores[-1].start()
    for store in stores:
        store.wait()


def local(image, sensitivity, system_blocks, tile_slab, tile_block, background):
    slabs, reps = lax.axis_size("slab"), lax.axis_size("rep")
    n = slabs * reps
    tiles, events, width = system_blocks.shape
    planes, rows, cols = image.shape
    block_rows = width // cols
    per_owner = rows // block_rows
    image2 = image.reshape(planes * rows, cols)
    sens2 = sensitivity.reshape(planes * rows, cols)
    sub = width // LANES

    vmem = pl.BlockSpec(memory_space=pltpu.VMEM)
    hbm = pl.BlockSpec(memory_space=pltpu.HBM)
    asked, scale, back = pl.pallas_call(
        functools.partial(exchange_kernel, (n, reps, tiles, block_rows, per_owner)),
        out_shape=(
            jax.ShapeDtypeStruct((n, LANES), jnp.int32),
            jax.ShapeDtypeStruct((n, LANES), jnp.float32),
            jax.ShapeDtypeStruct((n * CAP, sub, LANES), jnp.int16),
        ),
        in_specs=[hbm] * 5,
        out_specs=(vmem, vmem, vmem),
        scratch_shapes=[
            pltpu.VMEM((1, tiles), jnp.int32),
            pltpu.VMEM((1, tiles), jnp.int32),
            pltpu.VMEM(background.shape, jnp.bfloat16),
            pltpu.VMEM((n, LANES), jnp.float32),
            pltpu.VMEM(image2.shape, jnp.float32),
            pltpu.VMEM((planes * per_owner, sub, LANES), jnp.bfloat16),
            pltpu.VMEM(system_blocks.shape, jnp.bfloat16),
            pltpu.VMEM((n, LANES), jnp.int32),
            pltpu.VMEM((8, LANES), jnp.int32),
            pltpu.SMEM((n, LANES), jnp.int32),
            pltpu.SMEM((8, LANES), jnp.int32),
            pltpu.SMEM((n, LANES), jnp.int32),
            pltpu.VMEM((n * CAP, sub, LANES), jnp.bfloat16),
            pltpu.VMEM((n * CAP, sub, LANES), jnp.bfloat16),
            pltpu.VMEM((tiles, sub, LANES), jnp.float32),
            pltpu.VMEM((tiles, sub, LANES), jnp.int16),
            pltpu.VMEM((n * CAP, sub, LANES), jnp.int16),
            pltpu.SemaphoreType.DMA((7,)),
            pltpu.SemaphoreType.DMA((2,)),
            pltpu.SemaphoreType.DMA((2,)),
            pltpu.SemaphoreType.DMA((2,)),
            pltpu.SemaphoreType.DMA((2,)),
        ],
        compiler_params=pltpu.CompilerParams(
            collective_id=0, has_side_effects=True, vmem_limit_bytes=67043328
        ),
    )(tile_slab.reshape(1, tiles), tile_block.reshape(1, tiles), image2, system_blocks, background)
    updated = pl.pallas_call(
        functools.partial(update_kernel, (n, tiles, block_rows)),
        out_shape=jax.ShapeDtypeStruct(image2.shape, jnp.float32),
        in_specs=[hbm] * 5,
        out_specs=hbm,
        scratch_shapes=[
            pltpu.SMEM(asked.shape, jnp.int32),
            pltpu.SMEM(scale.shape, jnp.float32),
            pltpu.VMEM(back.shape, back.dtype),
            pltpu.VMEM(image2.shape, jnp.float32),
            pltpu.VMEM(image2.shape, jnp.float32),
            pltpu.VMEM(image2.shape, jnp.float32),
            pltpu.VMEM((planes * per_owner, sub, LANES), jnp.float32),
            pltpu.SemaphoreType.DMA((5,)),
            pltpu.SemaphoreType.DMA((4,)),
        ],
        compiler_params=pltpu.CompilerParams(vmem_limit_bytes=67043328),
    )(asked, scale, back, image2, sens2)
    return updated.reshape(image.shape)


def solution(mesh):
    return jax.shard_map(
        local,
        mesh=mesh,
        in_specs=(
            P("slab", "rep", None),
            P("slab", "rep", None),
            P(("slab", "rep"), None, None),
            P(("slab", "rep"), None),
            P(("slab", "rep")),
            P(("slab", "rep"), None),
        ),
        out_specs=P("slab", "rep", None),
        check_vma=False,
    )
```

```python
import functools

import jax
import jax.numpy as jnp
from jax import lax
from jax.experimental import pallas as pl
from jax.experimental.pallas import tpu as pltpu
from jax.sharding import PartitionSpec as P

CAP = 6
LEVELS = 65535.0
HALF = 32768
LANES = 128
MESH = pl.DeviceIdType.MESH


def split(x, size):
    if size & (size - 1):
        return x // size, x % size
    return x >> (size.bit_length() - 1), x & (size - 1)


def exchange_kernel(
    sizes, slab_hbm, block_hbm, image_hbm, sys_hbm, bg_hbm, asked_ref, scale_ref, back_ref,
    slab_v, block_v, bg_v, scale_v, image_v, blocks_v, sys_v, mine_v, slot_v, mine_s, slot_s, asked_s, send_f, recv_f, sums_v, bp_v, send_b,
    local_sem, id_sem, fetch_sem, back_sem, scale_sem,
):
    n, reps, tiles, block_rows, per_owner = sizes
    me = lax.axis_index("slab") * reps + lax.axis_index("rep")
    lane_tiles = image_v.shape[1] // LANES

    def device(d):
        return (lax.div(d, reps), lax.rem(d, reps))

    load_sys = pltpu.make_async_copy(sys_hbm, sys_v, local_sem.at[0])
    load_image = pltpu.make_async_copy(image_hbm, image_v, local_sem.at[1])
    load_slab = pltpu.make_async_copy(slab_hbm, slab_v, local_sem.at[4])
    load_block = pltpu.make_async_copy(block_hbm, block_v, local_sem.at[5])
    load_bg = pltpu.make_async_copy(bg_hbm, bg_v, local_sem.at[6])
    for load in (load_slab, load_block, load_image, load_bg, load_sys):
        load.start()

    barrier = pltpu.get_barrier_semaphore()

    def greet(i, c):
        pl.semaphore_signal(barrier, inc=1, device_id=device(lax.rem(me + i, n)), device_id_type=MESH)
        return c

    lax.fori_loop(1, n, greet, 0)

    load_slab.wait()
    load_block.wait()
    block = block_v[...]
    plane, within = split(block, per_owner * reps)
    owner, offset = split(within, per_owner)
    key = slab_v[...] * reps + owner
    value = (plane * per_owner + offset) * tiles + lax.broadcasted_iota(jnp.int32, (1, tiles), 1) + 1
    hot = key == lax.broadcasted_iota(jnp.int32, (n, tiles), 0)
    square = (tiles, tiles)
    earlier = lax.broadcasted_iota(jnp.int32, square, 0) < lax.broadcasted_iota(jnp.int32, square, 1)
    rank = jnp.dot(
        jnp.where(hot, 1.0, 0.0).astype(jnp.bfloat16),
        jnp.where(earlier, 1.0, 0.0).astype(jnp.bfloat16),
        preferred_element_type=jnp.float32,
    ).astype(jnp.int32)
    lane = lax.broadcasted_iota(jnp.int32, (n, LANES), 1)

    def tabled(row, zero):
        table = jnp.full((n, LANES), zero)
        for k in range(CAP):
            picked = jnp.sum(jnp.where(hot & (rank == k), row, zero), axis=1, keepdims=True)
            table = jnp.where(lane == k, picked, table)
        return table

    mine_v[...] = tabled(value, jnp.int32(0))
    own_rank = jnp.sum(jnp.where(hot, rank, 0), axis=0, keepdims=True)
    away = key - me
    slot = jnp.where(away < 0, away + n, away) * CAP + own_rank
    slot_v[0:1, 0:tiles] = jnp.clip(slot, 0, n * CAP - 1)
    to_slot = pltpu.make_async_copy(slot_v, slot_s, local_sem.at[2])
    to_slot.start()
    to_mine = pltpu.make_async_copy(mine_v, mine_s, local_sem.at[3])
    to_mine.start()
    asked_ref[pl.ds(0, 1), :] = mine_v[pl.ds(me, 1), :]

    pl.semaphore_wait(barrier, n - 1)

    def id_copy(i):
        d = lax.rem(me + i, n)
        return pltpu.make_async_remote_copy(
            src_ref=mine_v.at[pl.ds(d, 1)], dst_ref=asked_ref.at[pl.ds(i, 1)],
            send_sem=id_sem.at[0], recv_sem=id_sem.at[1],
            device_id=device(d), device_id_type=MESH,
        )

    def send_ids(i, c):
        id_copy(i).start()
        return c

    lax.fori_loop(1, n, send_ids, 0)
    to_slot.wait()
    to_mine.wait()
    load_image.wait()
    per_group = 8 // block_rows

    def cut(g, c):
        rows = image_v[pl.ds(pl.multiple_of(g * 8, 8), 8), :].astype(jnp.bfloat16).astype(jnp.float32)
        for u in range(per_group):
            blocks_v[g * per_group + u] = jnp.concatenate(
                [
                    rows[u * block_rows:(u + 1) * block_rows, h * LANES:(h + 1) * LANES]
                    for h in range(lane_tiles)
                ],
                axis=0,
            ).astype(jnp.bfloat16)
        return c

    lax.fori_loop(0, image_v.shape[0] // 8, cut, 0, unroll=4)
    rest = asked_ref.at[pl.ds(1, n - 1)]
    pltpu.make_async_copy(rest, rest, id_sem.at[1]).wait()
    to_asked = pltpu.make_async_copy(asked_ref, asked_s, local_sem.at[2])
    to_asked.start()
    to_asked.wait()

    def served(i, k):
        return blocks_v[split(jnp.maximum(asked_s[i, k] - 1, 0), tiles)[0]]

    for k in range(CAP):
        recv_f[k] = served(0, k)

    def serve(i, c):
        for k in range(CAP):
            send_f[i * CAP + k] = served(i, k)
        span = pl.ds(i * CAP, CAP)
        pltpu.make_async_remote_copy(
            src_ref=send_f.at[span], dst_ref=recv_f.at[span],
            send_sem=fetch_sem.at[0], recv_sem=fetch_sem.at[1],
            device_id=device(lax.rem(me + n - i, n)), device_id_type=MESH,
        ).start()
        return c

    lax.fori_loop(1, n, serve, 0)
    load_bg.wait()
    background = jnp.transpose(bg_v[...].astype(jnp.float32))
    load_sys.wait()
    others = recv_f.at[pl.ds(CAP, (n - 1) * CAP)]
    pltpu.make_async_copy(others, others, fetch_sem.at[1]).wait()

    forward = jnp.zeros(background.shape, jnp.float32)
    tile_lane = lax.broadcasted_iota(jnp.int32, (1, tiles), 1)
    pieces = block_rows * lane_tiles
    places = [(p % block_rows) * lane_tiles + p // block_rows for p in range(pieces)]
    for t in range(tiles):
        cells = recv_f[slot_s[0, t]].astype(jnp.float32)
        total = None
        for p, q in enumerate(places):
            term = sys_v[t, :, q * LANES:(q + 1) * LANES].astype(jnp.float32) * cells[p:p + 1, :]
            total = term if total is None else total + term
        forward = jnp.where(tile_lane == t, jnp.sum(total, axis=1, keepdims=True), forward)
    inverse = jnp.transpose(1.0 / (forward + background)).astype(jnp.bfloat16)
    tops = []
    for t in range(tiles):
        back = jnp.dot(inverse, sys_v[t], preferred_element_type=jnp.float32)
        tile = jnp.concatenate([back[t:t + 1, q * LANES:(q + 1) * LANES] for q in places], axis=0)
        sums_v[t] = tile
        tops.append(jnp.max(tile, axis=0, keepdims=True))
    peak = jnp.maximum(jnp.max(jnp.concatenate(tops, axis=0), axis=1, keepdims=True), 1e-33)
    gain = LEVELS / peak
    peaks = jnp.transpose(peak)
    for t in range(tiles):
        level = jnp.round(sums_v[t] * gain[t:t + 1, :]).astype(jnp.int32) - HALF
        bp_v[t] = jnp.clip(level, -HALF, HALF - 1).astype(jnp.int16)
    scale_v[...] = tabled(peaks * (1.0 / LEVELS), jnp.float32(0))

    def routed(d, k):
        return bp_v[split(jnp.maximum(mine_s[d, k] - 1, 0), tiles)[1]]

    for k in range(CAP):
        back_ref[k] = routed(me, k)

    def give(i, c):
        d = lax.rem(me + i, n)
        for k in range(CAP):
            send_b[i * CAP + k] = routed(d, k)
        span = pl.ds(i * CAP, CAP)
        pltpu.make_async_remote_copy(
            src_ref=send_b.at[span], dst_ref=back_ref.at[span],
            send_sem=back_sem.at[0], recv_sem=back_sem.at[1],
            device_id=device(d), device_id_type=MESH,
        ).start()
        pltpu.make_async_remote_copy(
            src_ref=scale_v.at[pl.ds(d, 1)], dst_ref=scale_ref.at[pl.ds(i, 1)],
            send_sem=scale_sem.at[0], recv_sem=scale_sem.at[1],
            device_id=device(d), device_id_type=MESH,
        ).start()
        return c

    scale_ref[pl.ds(0, 1), :] = scale_v[pl.ds(me, 1), :]
    lax.fori_loop(1, n, give, 0)
    scaled = scale_ref.at[pl.ds(1, n - 1)]
    pltpu.make_async_copy(scaled, scaled, scale_sem.at[0]).wait()
    pltpu.make_async_copy(scaled, scaled, scale_sem.at[1]).wait()
    pltpu.make_async_copy(mine_v.at[pl.ds(1, n - 1)], mine_v.at[pl.ds(1, n - 1)], id_sem.at[0]).wait()
    sent = send_f.at[pl.ds(CAP, (n - 1) * CAP)]
    pltpu.make_async_copy(sent, sent, fetch_sem.at[0]).wait()
    given = send_b.at[pl.ds(CAP, (n - 1) * CAP)]
    pltpu.make_async_copy(given, given, back_sem.at[0]).wait()
    landed = back_ref.at[pl.ds(CAP, (n - 1) * CAP)]
    pltpu.make_async_copy(landed, landed, back_sem.at[1]).wait()


def update_kernel(
    sizes, asked_hbm, scale_hbm, back_hbm, image_hbm, sens_hbm, out_hbm,
    asked_s, scale_s, back_ref, image_ref, sens_ref, out_ref, sums_v, in_sem, out_sem,
):
    n, tiles, block_rows = sizes
    moves = ((asked_hbm, asked_s), (scale_hbm, scale_s), (back_hbm, back_ref), (image_hbm, image_ref), (sens_hbm, sens_ref))
    loads = [pltpu.make_async_copy(src, dst, in_sem.at[j]) for j, (src, dst) in enumerate(moves)]
    for load in loads:
        load.start()
    lane_tiles = out_ref.shape[1] // LANES
    per_group = 8 // block_rows
    sums_v[...] = jnp.zeros_like(sums_v)

    def add(i, k):
        if k == CAP:
            return
        value = asked_s[i, k]

        @pl.when(value > 0)
        def _():
            level = back_ref[i * CAP + k].astype(jnp.int32) + HALF
            sums_v[split(value - 1, tiles)[0]] += level.astype(jnp.float32) * scale_s[i, k]
            add(i, k + 1)

    def one(i, c):
        add(i, 0)
        return c

    for load in loads[:3]:
        load.wait()
    lax.fori_loop(0, n, one, 0)
    for load in loads[3:]:
        load.wait()

    def finish(g, c):
        rows = pl.ds(pl.multiple_of(g * 8, 8), 8)
        sums = [sums_v[g * per_group + u] for u in range(per_group)]
        for h in range(lane_tiles):
            cols = slice(h * LANES, (h + 1) * LANES)
            total = jnp.concatenate([s[h * block_rows:(h + 1) * block_rows] for s in sums], axis=0)
            out_ref[rows, cols] = image_ref[rows, cols] * total / sens_ref[rows, cols]
        return c

    groups = out_ref.shape[0] // 8
    chunks = out_sem.shape[0]
    stores = []
    for c in range(chunks):
        first, last = groups * c // chunks, groups * (c + 1) // chunks
        lax.fori_loop(first, last, finish, 0, unroll=4)
        span = pl.ds(first * 8, (last - first) * 8)
        stores.append(pltpu.make_async_copy(out_ref.at[span], out_hbm.at[span], out_sem.at[c]))
        stores[-1].start()
    for store in stores:
        store.wait()


def local(image, sensitivity, system_blocks, tile_slab, tile_block, background):
    slabs, reps = lax.axis_size("slab"), lax.axis_size("rep")
    n = slabs * reps
    tiles, events, width = system_blocks.shape
    planes, rows, cols = image.shape
    block_rows = width // cols
    per_owner = rows // block_rows
    image2 = image.reshape(planes * rows, cols)
    sens2 = sensitivity.reshape(planes * rows, cols)
    sub = width // LANES

    vmem = pl.BlockSpec(memory_space=pltpu.VMEM)
    hbm = pl.BlockSpec(memory_space=pltpu.HBM)
    asked, scale, back = pl.pallas_call(
        functools.partial(exchange_kernel, (n, reps, tiles, block_rows, per_owner)),
        out_shape=(
            jax.ShapeDtypeStruct((n, LANES), jnp.int32),
            jax.ShapeDtypeStruct((n, LANES), jnp.float32),
            jax.ShapeDtypeStruct((n * CAP, sub, LANES), jnp.int16),
        ),
        in_specs=[hbm] * 5,
        out_specs=(vmem, vmem, vmem),
        scratch_shapes=[
            pltpu.VMEM((1, tiles), jnp.int32),
            pltpu.VMEM((1, tiles), jnp.int32),
            pltpu.VMEM(background.shape, jnp.bfloat16),
            pltpu.VMEM((n, LANES), jnp.float32),
            pltpu.VMEM(image2.shape, jnp.float32),
            pltpu.VMEM((planes * per_owner, sub, LANES), jnp.bfloat16),
            pltpu.VMEM(system_blocks.shape, jnp.bfloat16),
            pltpu.VMEM((n, LANES), jnp.int32),
            pltpu.VMEM((8, LANES), jnp.int32),
            pltpu.SMEM((n, LANES), jnp.int32),
            pltpu.SMEM((8, LANES), jnp.int32),
            pltpu.SMEM((n, LANES), jnp.int32),
            pltpu.VMEM((n * CAP, sub, LANES), jnp.bfloat16),
            pltpu.VMEM((n * CAP, sub, LANES), jnp.bfloat16),
            pltpu.VMEM((tiles, sub, LANES), jnp.float32),
            pltpu.VMEM((tiles, sub, LANES), jnp.int16),
            pltpu.VMEM((n * CAP, sub, LANES), jnp.int16),
            pltpu.SemaphoreType.DMA((7,)),
            pltpu.SemaphoreType.DMA((2,)),
            pltpu.SemaphoreType.DMA((2,)),
            pltpu.SemaphoreType.DMA((2,)),
            pltpu.SemaphoreType.DMA((2,)),
        ],
        compiler_params=pltpu.CompilerParams(
            collective_id=0, has_side_effects=True, vmem_limit_bytes=67043328
        ),
    )(tile_slab.reshape(1, tiles), tile_block.reshape(1, tiles), image2, system_blocks, background)
    updated = pl.pallas_call(
        functools.partial(update_kernel, (n, tiles, block_rows)),
        out_shape=jax.ShapeDtypeStruct(image2.shape, jnp.float32),
        in_specs=[hbm] * 5,
        out_specs=hbm,
        scratch_shapes=[
            pltpu.SMEM(asked.shape, jnp.int32),
            pltpu.SMEM(scale.shape, jnp.float32),
            pltpu.VMEM(back.shape, back.dtype),
            pltpu.VMEM(image2.shape, jnp.float32),
            pltpu.VMEM(image2.shape, jnp.float32),
            pltpu.VMEM(image2.shape, jnp.float32),
            pltpu.VMEM((planes * per_owner, sub, LANES), jnp.float32),
            pltpu.SemaphoreType.DMA((5,)),
            pltpu.SemaphoreType.DMA((4,)),
        ],
        compiler_params=pltpu.CompilerParams(vmem_limit_bytes=67043328),
    )(asked, scale, back, image2, sens2)
    return updated.reshape(image.shape)


def solution(mesh):
    return jax.shard_map(
        local,
        mesh=mesh,
        in_specs=(
            P("slab", "rep", None),
            P("slab", "rep", None),
            P(("slab", "rep"), None, None),
            P(("slab", "rep"), None),
            P(("slab", "rep")),
            P(("slab", "rep"), None),
        ),
        out_specs=P("slab", "rep", None),
        check_vma=False,
    )
```

```python
import functools

import jax
import jax.numpy as jnp
from jax import lax
from jax.experimental import pallas as pl
from jax.experimental.pallas import tpu as pltpu
from jax.sharding import PartitionSpec as P

CAP = 6
LEVELS = 65535.0
HALF = 32768
LANES = 128
MESH = pl.DeviceIdType.MESH


def split(x, size):
    if size & (size - 1):
        return x // size, x % size
    return x >> (size.bit_length() - 1), x & (size - 1)


def exchange_kernel(
    sizes, slab_hbm, block_hbm, image_hbm, sys_hbm, bg_hbm, asked_hbm, scale_ref, back_ref,
    asked_ref, slab_v, block_v, bg_v, scale_v, image_v, blocks_v, sys_v, mine_v, slot_v, mine_s, slot_s, asked_s, send_f, recv_f, sums_v, bp_v, send_b,
    local_sem, id_sem, fetch_sem, back_sem, scale_sem,
):
    n, reps, tiles, block_rows, per_owner = sizes
    me = lax.axis_index("slab") * reps + lax.axis_index("rep")
    lane_tiles = image_v.shape[1] // LANES

    def device(d):
        return (lax.div(d, reps), lax.rem(d, reps))

    load_sys = pltpu.make_async_copy(sys_hbm, sys_v, local_sem.at[0])
    load_image = pltpu.make_async_copy(image_hbm, image_v, local_sem.at[1])
    load_slab = pltpu.make_async_copy(slab_hbm, slab_v, local_sem.at[4])
    load_block = pltpu.make_async_copy(block_hbm, block_v, local_sem.at[5])
    load_bg = pltpu.make_async_copy(bg_hbm, bg_v, local_sem.at[6])
    for load in (load_slab, load_block, load_image, load_bg, load_sys):
        load.start()

    barrier = pltpu.get_barrier_semaphore()

    def greet(i, c):
        pl.semaphore_signal(barrier, inc=1, device_id=device(lax.rem(me + i, n)), device_id_type=MESH)
        return c

    lax.fori_loop(1, n, greet, 0)

    load_slab.wait()
    load_block.wait()
    block = block_v[...]
    plane, within = split(block, per_owner * reps)
    owner, offset = split(within, per_owner)
    key = slab_v[...] * reps + owner
    value = (plane * per_owner + offset) * tiles + lax.broadcasted_iota(jnp.int32, (1, tiles), 1) + 1
    hot = key == lax.broadcasted_iota(jnp.int32, (n, tiles), 0)
    square = (tiles, tiles)
    earlier = lax.broadcasted_iota(jnp.int32, square, 0) < lax.broadcasted_iota(jnp.int32, square, 1)
    rank = jnp.dot(
        jnp.where(hot, 1.0, 0.0).astype(jnp.bfloat16),
        jnp.where(earlier, 1.0, 0.0).astype(jnp.bfloat16),
        preferred_element_type=jnp.float32,
    ).astype(jnp.int32)
    lane = lax.broadcasted_iota(jnp.int32, (n, LANES), 1)

    def tabled(row, zero):
        table = jnp.full((n, LANES), zero)
        for k in range(CAP):
            picked = jnp.sum(jnp.where(hot & (rank == k), row, zero), axis=1, keepdims=True)
            table = jnp.where(lane == k, picked, table)
        return table

    mine_v[...] = tabled(value, jnp.int32(0))
    own_rank = jnp.sum(jnp.where(hot, rank, 0), axis=0, keepdims=True)
    away = key - me
    slot = jnp.where(away < 0, away + n, away) * CAP + own_rank
    slot_v[0:1, 0:tiles] = jnp.clip(slot, 0, n * CAP - 1)
    to_slot = pltpu.make_async_copy(slot_v, slot_s, local_sem.at[2])
    to_slot.start()
    to_mine = pltpu.make_async_copy(mine_v, mine_s, local_sem.at[3])
    to_mine.start()
    asked_ref[pl.ds(0, 1), :] = mine_v[pl.ds(me, 1), :]

    pl.semaphore_wait(barrier, n - 1)

    def id_copy(i):
        d = lax.rem(me + i, n)
        return pltpu.make_async_remote_copy(
            src_ref=mine_v.at[pl.ds(d, 1)], dst_ref=asked_ref.at[pl.ds(i, 1)],
            send_sem=id_sem.at[0], recv_sem=id_sem.at[1],
            device_id=device(d), device_id_type=MESH,
        )

    def send_ids(i, c):
        id_copy(i).start()
        return c

    lax.fori_loop(1, n, send_ids, 0)
    to_slot.wait()
    to_mine.wait()
    load_image.wait()
    per_group = 8 // block_rows

    def cut(g, c):
        rows = image_v[pl.ds(pl.multiple_of(g * 8, 8), 8), :].astype(jnp.bfloat16).astype(jnp.float32)
        for u in range(per_group):
            blocks_v[g * per_group + u] = jnp.concatenate(
                [
                    rows[u * block_rows:(u + 1) * block_rows, h * LANES:(h + 1) * LANES]
                    for h in range(lane_tiles)
                ],
                axis=0,
            ).astype(jnp.bfloat16)
        return c

    lax.fori_loop(0, image_v.shape[0] // 8, cut, 0, unroll=4)
    rest = asked_ref.at[pl.ds(1, n - 1)]
    pltpu.make_async_copy(rest, rest, id_sem.at[1]).wait()
    to_asked = pltpu.make_async_copy(asked_ref, asked_s, local_sem.at[2])
    to_asked.start()
    keep_asked = pltpu.make_async_copy(asked_ref, asked_hbm, local_sem.at[3])
    keep_asked.start()
    to_asked.wait()

    def served(i, k):
        return blocks_v[split(jnp.maximum(asked_s[i, k] - 1, 0), tiles)[0]]

    for k in range(CAP):
        recv_f[k] = served(0, k)

    def serve(i, c):
        for k in range(CAP):
            send_f[i * CAP + k] = served(i, k)
        span = pl.ds(i * CAP, CAP)
        pltpu.make_async_remote_copy(
            src_ref=send_f.at[span], dst_ref=recv_f.at[span],
            send_sem=fetch_sem.at[0], recv_sem=fetch_sem.at[1],
            device_id=device(lax.rem(me + n - i, n)), device_id_type=MESH,
        ).start()
        return c

    lax.fori_loop(1, n, serve, 0)
    load_bg.wait()
    background = jnp.transpose(bg_v[...].astype(jnp.float32))
    load_sys.wait()
    others = recv_f.at[pl.ds(CAP, (n - 1) * CAP)]
    pltpu.make_async_copy(others, others, fetch_sem.at[1]).wait()

    forward = jnp.zeros(background.shape, jnp.float32)
    tile_lane = lax.broadcasted_iota(jnp.int32, (1, tiles), 1)
    pieces = block_rows * lane_tiles
    places = [(p % block_rows) * lane_tiles + p // block_rows for p in range(pieces)]
    for t in range(tiles):
        cells = recv_f[slot_s[0, t]].astype(jnp.float32)
        total = None
        for p, q in enumerate(places):
            term = sys_v[t, :, q * LANES:(q + 1) * LANES].astype(jnp.float32) * cells[p:p + 1, :]
            total = term if total is None else total + term
        forward = jnp.where(tile_lane == t, jnp.sum(total, axis=1, keepdims=True), forward)
    inverse = jnp.transpose(1.0 / (forward + background)).astype(jnp.bfloat16)
    tops = []
    for t in range(tiles):
        back = jnp.dot(inverse, sys_v[t], preferred_element_type=jnp.float32)
        tile = jnp.concatenate([back[t:t + 1, q * LANES:(q + 1) * LANES] for q in places], axis=0)
        sums_v[t] = tile
        tops.append(jnp.max(tile, axis=0, keepdims=True))
    peak = jnp.maximum(jnp.max(jnp.concatenate(tops, axis=0), axis=1, keepdims=True), 1e-33)
    gain = LEVELS / peak
    peaks = jnp.transpose(peak)
    for t in range(tiles):
        level = jnp.round(sums_v[t] * gain[t:t + 1, :]).astype(jnp.int32) - HALF
        bp_v[t] = jnp.clip(level, -HALF, HALF - 1).astype(jnp.int16)
    scale_v[...] = tabled(peaks * (1.0 / LEVELS), jnp.float32(0))

    def routed(d, k):
        return bp_v[split(jnp.maximum(mine_s[d, k] - 1, 0), tiles)[1]]

    for k in range(CAP):
        send_b[k] = routed(me, k)
    own_back = pltpu.make_async_copy(send_b.at[pl.ds(0, CAP)], back_ref.at[pl.ds(0, CAP)], local_sem.at[4])
    own_back.start()
    own_scale = pltpu.make_async_copy(scale_v.at[pl.ds(me, 1)], scale_ref.at[pl.ds(0, 1)], local_sem.at[5])
    own_scale.start()

    def give(i, c):
        d = lax.rem(me + i, n)
        for k in range(CAP):
            send_b[i * CAP + k] = routed(d, k)
        span = pl.ds(i * CAP, CAP)
        pltpu.make_async_remote_copy(
            src_ref=send_b.at[span], dst_ref=back_ref.at[span],
            send_sem=back_sem.at[0], recv_sem=back_sem.at[1],
            device_id=device(d), device_id_type=MESH,
        ).start()
        pltpu.make_async_remote_copy(
            src_ref=scale_v.at[pl.ds(d, 1)], dst_ref=scale_ref.at[pl.ds(i, 1)],
            send_sem=scale_sem.at[0], recv_sem=scale_sem.at[1],
            device_id=device(d), device_id_type=MESH,
        ).start()
        return c

    lax.fori_loop(1, n, give, 0)
    for copy in (keep_asked, own_back, own_scale):
        copy.wait()
    scaled = scale_ref.at[pl.ds(1, n - 1)]
    pltpu.make_async_copy(scaled, scaled, scale_sem.at[0]).wait()
    pltpu.make_async_copy(scaled, scaled, scale_sem.at[1]).wait()
    pltpu.make_async_copy(mine_v.at[pl.ds(1, n - 1)], mine_v.at[pl.ds(1, n - 1)], id_sem.at[0]).wait()
    sent = send_f.at[pl.ds(CAP, (n - 1) * CAP)]
    pltpu.make_async_copy(sent, sent, fetch_sem.at[0]).wait()
    given = send_b.at[pl.ds(CAP, (n - 1) * CAP)]
    pltpu.make_async_copy(given, given, back_sem.at[0]).wait()
    landed = back_ref.at[pl.ds(CAP, (n - 1) * CAP)]
    pltpu.make_async_copy(landed, landed, back_sem.at[1]).wait()


def update_kernel(
    sizes, asked_hbm, scale_hbm, back_hbm, image_hbm, sens_hbm, out_hbm,
    asked_s, scale_s, back_ref, image_ref, sens_ref, out_ref, sums_v, in_sem, out_sem,
):
    n, tiles, block_rows = sizes
    moves = ((asked_hbm, asked_s), (scale_hbm, scale_s), (back_hbm, back_ref), (image_hbm, image_ref), (sens_hbm, sens_ref))
    loads = [pltpu.make_async_copy(src, dst, in_sem.at[j]) for j, (src, dst) in enumerate(moves)]
    for load in loads:
        load.start()
    lane_tiles = out_ref.shape[1] // LANES
    per_group = 8 // block_rows
    sums_v[...] = jnp.zeros_like(sums_v)

    def add(i, k):
        if k == CAP:
            return
        value = asked_s[i, k]

        @pl.when(value > 0)
        def _():
            level = back_ref[i * CAP + k].astype(jnp.int32) + HALF
            sums_v[split(value - 1, tiles)[0]] += level.astype(jnp.float32) * scale_s[i, k]
            add(i, k + 1)

    def one(i, c):
        add(i, 0)
        return c

    for load in loads[:3]:
        load.wait()
    lax.fori_loop(0, n, one, 0)
    for load in loads[3:]:
        load.wait()

    def finish(g, c):
        rows = pl.ds(pl.multiple_of(g * 8, 8), 8)
        sums = [sums_v[g * per_group + u] for u in range(per_group)]
        for h in range(lane_tiles):
            cols = slice(h * LANES, (h + 1) * LANES)
            total = jnp.concatenate([s[h * block_rows:(h + 1) * block_rows] for s in sums], axis=0)
            out_ref[rows, cols] = image_ref[rows, cols] * total / sens_ref[rows, cols]
        return c

    groups = out_ref.shape[0] // 8
    chunks = out_sem.shape[0]
    stores = []
    for c in range(chunks):
        first, last = groups * c // chunks, groups * (c + 1) // chunks
        lax.fori_loop(first, last, finish, 0, unroll=4)
        span = pl.ds(first * 8, (last - first) * 8)
        stores.append(pltpu.make_async_copy(out_ref.at[span], out_hbm.at[span], out_sem.at[c]))
        stores[-1].start()
    for store in stores:
        store.wait()


def local(image, sensitivity, system_blocks, tile_slab, tile_block, background):
    slabs, reps = lax.axis_size("slab"), lax.axis_size("rep")
    n = slabs * reps
    tiles, events, width = system_blocks.shape
    planes, rows, cols = image.shape
    block_rows = width // cols
    per_owner = rows // block_rows
    image2 = image.reshape(planes * rows, cols)
    sens2 = sensitivity.reshape(planes * rows, cols)
    sub = width // LANES

    hbm = pl.BlockSpec(memory_space=pltpu.HBM)
    asked, scale, back = pl.pallas_call(
        functools.partial(exchange_kernel, (n, reps, tiles, block_rows, per_owner)),
        out_shape=(
            jax.ShapeDtypeStruct((n, LANES), jnp.int32),
            jax.ShapeDtypeStruct((n, LANES), jnp.float32),
            jax.ShapeDtypeStruct((n * CAP, sub, LANES), jnp.int16),
        ),
        in_specs=[hbm] * 5,
        out_specs=(hbm, hbm, hbm),
        scratch_shapes=[
            pltpu.VMEM((n, LANES), jnp.int32),
            pltpu.VMEM((1, tiles), jnp.int32),
            pltpu.VMEM((1, tiles), jnp.int32),
            pltpu.VMEM(background.shape, jnp.bfloat16),
            pltpu.VMEM((n, LANES), jnp.float32),
            pltpu.VMEM(image2.shape, jnp.float32),
            pltpu.VMEM((planes * per_owner, sub, LANES), jnp.bfloat16),
            pltpu.VMEM(system_blocks.shape, jnp.bfloat16),
            pltpu.VMEM((n, LANES), jnp.int32),
            pltpu.VMEM((8, LANES), jnp.int32),
            pltpu.SMEM((n, LANES), jnp.int32),
            pltpu.SMEM((8, LANES), jnp.int32),
            pltpu.SMEM((n, LANES), jnp.int32),
            pltpu.VMEM((n * CAP, sub, LANES), jnp.bfloat16),
            pltpu.VMEM((n * CAP, sub, LANES), jnp.bfloat16),
            pltpu.VMEM((tiles, sub, LANES), jnp.float32),
            pltpu.VMEM((tiles, sub, LANES), jnp.int16),
            pltpu.VMEM((n * CAP, sub, LANES), jnp.int16),
            pltpu.SemaphoreType.DMA((7,)),
            pltpu.SemaphoreType.DMA((2,)),
            pltpu.SemaphoreType.DMA((2,)),
            pltpu.SemaphoreType.DMA((2,)),
            pltpu.SemaphoreType.DMA((2,)),
        ],
        compiler_params=pltpu.CompilerParams(
            collective_id=0, has_side_effects=True, vmem_limit_bytes=67043328
        ),
    )(tile_slab.reshape(1, tiles), tile_block.reshape(1, tiles), image2, system_blocks, background)
    updated = pl.pallas_call(
        functools.partial(update_kernel, (n, tiles, block_rows)),
        out_shape=jax.ShapeDtypeStruct(image2.shape, jnp.float32),
        in_specs=[hbm] * 5,
        out_specs=hbm,
        scratch_shapes=[
            pltpu.SMEM(asked.shape, jnp.int32),
            pltpu.SMEM(scale.shape, jnp.float32),
            pltpu.VMEM(back.shape, back.dtype),
            pltpu.VMEM(image2.shape, jnp.float32),
            pltpu.VMEM(image2.shape, jnp.float32),
            pltpu.VMEM(image2.shape, jnp.float32),
            pltpu.VMEM((planes * per_owner, sub, LANES), jnp.float32),
            pltpu.SemaphoreType.DMA((5,)),
            pltpu.SemaphoreType.DMA((4,)),
        ],
        compiler_params=pltpu.CompilerParams(vmem_limit_bytes=67043328),
    )(asked, scale, back, image2, sens2)
    return updated.reshape(image.shape)


def solution(mesh):
    return jax.shard_map(
        local,
        mesh=mesh,
        in_specs=(
            P("slab", "rep", None),
            P("slab", "rep", None),
            P(("slab", "rep"), None, None),
            P(("slab", "rep"), None),
            P(("slab", "rep")),
            P(("slab", "rep"), None),
        ),
        out_specs=P("slab", "rep", None),
        check_vma=False,
    )
```

```python
import functools

import jax
import jax.numpy as jnp
from jax import lax
from jax.experimental import pallas as pl
from jax.experimental.pallas import tpu as pltpu
from jax.sharding import PartitionSpec as P

CAP = 6
LEVELS = 65535.0
HALF = 32768
LANES = 128
MESH = pl.DeviceIdType.MESH


def split(x, size):
    if size & (size - 1):
        return x // size, x % size
    return x >> (size.bit_length() - 1), x & (size - 1)


def exchange_kernel(
    sizes, slab_hbm, block_hbm, image_hbm, sys_hbm, bg_hbm, asked_hbm, scale_ref, back_ref,
    asked_ref, slab_v, block_v, bg_v, scale_v, image_v, blocks_v, sys_v, mine_v, slot_v, mine_s, slot_s, asked_s, send_f, recv_f, sums_v, bp_v, send_b,
    local_sem, id_sem, fetch_sem, back_sem, scale_sem,
):
    n, reps, tiles, block_rows, per_owner = sizes
    me = lax.axis_index("slab") * reps + lax.axis_index("rep")
    lane_tiles = image_v.shape[1] // LANES

    def device(d):
        return (lax.div(d, reps), lax.rem(d, reps))

    load_sys = pltpu.make_async_copy(sys_hbm, sys_v, local_sem.at[0])
    load_image = pltpu.make_async_copy(image_hbm, image_v, local_sem.at[1])
    load_slab = pltpu.make_async_copy(slab_hbm, slab_v, local_sem.at[4])
    load_block = pltpu.make_async_copy(block_hbm, block_v, local_sem.at[5])
    load_bg = pltpu.make_async_copy(bg_hbm, bg_v, local_sem.at[6])
    for load in (load_slab, load_block, load_image, load_bg, load_sys):
        load.start()

    barrier = pltpu.get_barrier_semaphore()

    def greet(i, c):
        pl.semaphore_signal(barrier, inc=1, device_id=device(lax.rem(me + i, n)), device_id_type=MESH)
        return c

    lax.fori_loop(1, n, greet, 0)

    load_slab.wait()
    load_block.wait()
    block = block_v[...]
    plane, within = split(block, per_owner * reps)
    owner, offset = split(within, per_owner)
    key = slab_v[...] * reps + owner
    value = (plane * per_owner + offset) * tiles + lax.broadcasted_iota(jnp.int32, (1, tiles), 1) + 1
    hot = key == lax.broadcasted_iota(jnp.int32, (n, tiles), 0)
    square = (tiles, tiles)
    earlier = lax.broadcasted_iota(jnp.int32, square, 0) < lax.broadcasted_iota(jnp.int32, square, 1)
    rank = jnp.dot(
        jnp.where(hot, 1.0, 0.0).astype(jnp.bfloat16),
        jnp.where(earlier, 1.0, 0.0).astype(jnp.bfloat16),
        preferred_element_type=jnp.float32,
    ).astype(jnp.int32)
    lane = lax.broadcasted_iota(jnp.int32, (n, LANES), 1)

    def tabled(row, zero):
        table = jnp.full((n, LANES), zero)
        for k in range(CAP):
            picked = jnp.sum(jnp.where(hot & (rank == k), row, zero), axis=1, keepdims=True)
            table = jnp.where(lane == k, picked, table)
        return table

    mine_v[...] = tabled(value, jnp.int32(0))
    own_rank = jnp.sum(jnp.where(hot, rank, 0), axis=0, keepdims=True)
    away = key - me
    slot = jnp.where(away < 0, away + n, away) * CAP + own_rank
    slot_v[0:1, 0:tiles] = jnp.clip(slot, 0, n * CAP - 1)
    to_slot = pltpu.make_async_copy(slot_v, slot_s, local_sem.at[2])
    to_slot.start()
    to_mine = pltpu.make_async_copy(mine_v, mine_s, local_sem.at[3])
    to_mine.start()
    asked_ref[pl.ds(0, 1), :] = mine_v[pl.ds(me, 1), :]

    pl.semaphore_wait(barrier, n - 1)

    def id_copy(i):
        d = lax.rem(me + i, n)
        return pltpu.make_async_remote_copy(
            src_ref=mine_v.at[pl.ds(d, 1)], dst_ref=asked_ref.at[pl.ds(i, 1)],
            send_sem=id_sem.at[0], recv_sem=id_sem.at[1],
            device_id=device(d), device_id_type=MESH,
        )

    def send_ids(i, c):
        id_copy(i).start()
        return c

    lax.fori_loop(1, n, send_ids, 0)
    to_slot.wait()
    to_mine.wait()
    load_image.wait()
    per_group = 8 // block_rows

    def cut(g, c):
        rows = image_v[pl.ds(pl.multiple_of(g * 8, 8), 8), :].astype(jnp.bfloat16).astype(jnp.float32)
        for u in range(per_group):
            blocks_v[g * per_group + u] = jnp.concatenate(
                [
                    rows[u * block_rows:(u + 1) * block_rows, h * LANES:(h + 1) * LANES]
                    for h in range(lane_tiles)
                ],
                axis=0,
            ).astype(jnp.bfloat16)
        return c

    lax.fori_loop(0, image_v.shape[0] // 8, cut, 0, unroll=4)
    rest = asked_ref.at[pl.ds(1, n - 1)]
    pltpu.make_async_copy(rest, rest, id_sem.at[1]).wait()
    to_asked = pltpu.make_async_copy(asked_ref, asked_s, local_sem.at[2])
    to_asked.start()
    keep_asked = pltpu.make_async_copy(asked_ref, asked_hbm, local_sem.at[3])
    keep_asked.start()
    to_asked.wait()

    def served(i, k):
        return blocks_v[split(jnp.maximum(asked_s[i, k] - 1, 0), tiles)[0]]

    for k in range(CAP):
        recv_f[k] = served(0, k)

    def far_first(j):
        return lax.rem(j, slabs) * reps + lax.rem(reps // 2 + lax.div(j, slabs), reps)

    slabs = n // reps
    own_turn = (reps - reps // 2) * slabs

    def serve(j, c):
        i = far_first(j)
        for k in range(CAP):
            send_f[i * CAP + k] = served(i, k)
        span = pl.ds(i * CAP, CAP)
        pltpu.make_async_remote_copy(
            src_ref=send_f.at[span], dst_ref=recv_f.at[span],
            send_sem=fetch_sem.at[0], recv_sem=fetch_sem.at[1],
            device_id=device(lax.rem(me + n - i, n)), device_id_type=MESH,
        ).start()
        return c

    lax.fori_loop(0, own_turn, serve, 0)
    lax.fori_loop(own_turn + 1, n, serve, 0)
    load_bg.wait()
    background = jnp.transpose(bg_v[...].astype(jnp.float32))
    load_sys.wait()
    others = recv_f.at[pl.ds(CAP, (n - 1) * CAP)]
    pltpu.make_async_copy(others, others, fetch_sem.at[1]).wait()

    forward = jnp.zeros(background.shape, jnp.float32)
    tile_lane = lax.broadcasted_iota(jnp.int32, (1, tiles), 1)
    pieces = block_rows * lane_tiles
    places = [(p % block_rows) * lane_tiles + p // block_rows for p in range(pieces)]
    for t in range(tiles):
        cells = recv_f[slot_s[0, t]].astype(jnp.float32)
        total = None
        for p, q in enumerate(places):
            term = sys_v[t, :, q * LANES:(q + 1) * LANES].astype(jnp.float32) * cells[p:p + 1, :]
            total = term if total is None else total + term
        forward = jnp.where(tile_lane == t, jnp.sum(total, axis=1, keepdims=True), forward)
    inverse = jnp.transpose(1.0 / (forward + background)).astype(jnp.bfloat16)
    tops = []
    for t in range(tiles):
        back = jnp.dot(inverse, sys_v[t], preferred_element_type=jnp.float32)
        tile = jnp.concatenate([back[t:t + 1, q * LANES:(q + 1) * LANES] for q in places], axis=0)
        sums_v[t] = tile
        tops.append(jnp.max(tile, axis=0, keepdims=True))
    peak = jnp.maximum(jnp.max(jnp.concatenate(tops, axis=0), axis=1, keepdims=True), 1e-33)
    gain = LEVELS / peak
    peaks = jnp.transpose(peak)
    for t in range(tiles):
        level = jnp.round(sums_v[t] * gain[t:t + 1, :]).astype(jnp.int32) - HALF
        bp_v[t] = jnp.clip(level, -HALF, HALF - 1).astype(jnp.int16)
    scale_v[...] = tabled(peaks * (1.0 / LEVELS), jnp.float32(0))

    def routed(d, k):
        return bp_v[split(jnp.maximum(mine_s[d, k] - 1, 0), tiles)[1]]

    for k in range(CAP):
        send_b[k] = routed(me, k)
    own_back = pltpu.make_async_copy(send_b.at[pl.ds(0, CAP)], back_ref.at[pl.ds(0, CAP)], local_sem.at[4])
    own_back.start()
    own_scale = pltpu.make_async_copy(scale_v.at[pl.ds(me, 1)], scale_ref.at[pl.ds(0, 1)], local_sem.at[5])
    own_scale.start()

    def give(j, c):
        i = far_first(j)
        d = lax.rem(me + i, n)
        for k in range(CAP):
            send_b[i * CAP + k] = routed(d, k)
        span = pl.ds(i * CAP, CAP)
        pltpu.make_async_remote_copy(
            src_ref=send_b.at[span], dst_ref=back_ref.at[span],
            send_sem=back_sem.at[0], recv_sem=back_sem.at[1],
            device_id=device(d), device_id_type=MESH,
        ).start()
        pltpu.make_async_remote_copy(
            src_ref=scale_v.at[pl.ds(d, 1)], dst_ref=scale_ref.at[pl.ds(i, 1)],
            send_sem=scale_sem.at[0], recv_sem=scale_sem.at[1],
            device_id=device(d), device_id_type=MESH,
        ).start()
        return c

    lax.fori_loop(0, own_turn, give, 0)
    lax.fori_loop(own_turn + 1, n, give, 0)
    for copy in (keep_asked, own_back, own_scale):
        copy.wait()
    scaled = scale_ref.at[pl.ds(1, n - 1)]
    pltpu.make_async_copy(scaled, scaled, scale_sem.at[0]).wait()
    pltpu.make_async_copy(scaled, scaled, scale_sem.at[1]).wait()
    pltpu.make_async_copy(mine_v.at[pl.ds(1, n - 1)], mine_v.at[pl.ds(1, n - 1)], id_sem.at[0]).wait()
    sent = send_f.at[pl.ds(CAP, (n - 1) * CAP)]
    pltpu.make_async_copy(sent, sent, fetch_sem.at[0]).wait()
    given = send_b.at[pl.ds(CAP, (n - 1) * CAP)]
    pltpu.make_async_copy(given, given, back_sem.at[0]).wait()
    landed = back_ref.at[pl.ds(CAP, (n - 1) * CAP)]
    pltpu.make_async_copy(landed, landed, back_sem.at[1]).wait()


def update_kernel(
    sizes, asked_hbm, scale_hbm, back_hbm, image_hbm, sens_hbm, out_hbm,
    asked_s, scale_s, back_ref, image_ref, sens_ref, out_ref, sums_v, in_sem, out_sem,
):
    n, tiles, block_rows = sizes
    moves = ((asked_hbm, asked_s), (scale_hbm, scale_s), (back_hbm, back_ref), (image_hbm, image_ref), (sens_hbm, sens_ref))
    loads = [pltpu.make_async_copy(src, dst, in_sem.at[j]) for j, (src, dst) in enumerate(moves)]
    for load in loads:
        load.start()
    lane_tiles = out_ref.shape[1] // LANES
    per_group = 8 // block_rows
    sums_v[...] = jnp.zeros_like(sums_v)

    def add(i, k):
        if k == CAP:
            return
        value = asked_s[i, k]

        @pl.when(value > 0)
        def _():
            level = back_ref[i * CAP + k].astype(jnp.int32) + HALF
            sums_v[split(value - 1, tiles)[0]] += level.astype(jnp.float32) * scale_s[i, k]
            add(i, k + 1)

    def one(i, c):
        add(i, 0)
        return c

    for load in loads[:3]:
        load.wait()
    lax.fori_loop(0, n, one, 0)
    for load in loads[3:]:
        load.wait()

    def finish(g, c):
        rows = pl.ds(pl.multiple_of(g * 8, 8), 8)
        sums = [sums_v[g * per_group + u] for u in range(per_group)]
        for h in range(lane_tiles):
            cols = slice(h * LANES, (h + 1) * LANES)
            total = jnp.concatenate([s[h * block_rows:(h + 1) * block_rows] for s in sums], axis=0)
            out_ref[rows, cols] = image_ref[rows, cols] * total / sens_ref[rows, cols]
        return c

    groups = out_ref.shape[0] // 8
    chunks = out_sem.shape[0]
    stores = []
    for c in range(chunks):
        first, last = groups * c // chunks, groups * (c + 1) // chunks
        lax.fori_loop(first, last, finish, 0, unroll=4)
        span = pl.ds(first * 8, (last - first) * 8)
        stores.append(pltpu.make_async_copy(out_ref.at[span], out_hbm.at[span], out_sem.at[c]))
        stores[-1].start()
    for store in stores:
        store.wait()


def local(image, sensitivity, system_blocks, tile_slab, tile_block, background):
    slabs, reps = lax.axis_size("slab"), lax.axis_size("rep")
    n = slabs * reps
    tiles, events, width = system_blocks.shape
    planes, rows, cols = image.shape
    block_rows = width // cols
    per_owner = rows // block_rows
    image2 = image.reshape(planes * rows, cols)
    sens2 = sensitivity.reshape(planes * rows, cols)
    sub = width // LANES

    hbm = pl.BlockSpec(memory_space=pltpu.HBM)
    asked, scale, back = pl.pallas_call(
        functools.partial(exchange_kernel, (n, reps, tiles, block_rows, per_owner)),
        out_shape=(
            jax.ShapeDtypeStruct((n, LANES), jnp.int32),
            jax.ShapeDtypeStruct((n, LANES), jnp.float32),
            jax.ShapeDtypeStruct((n * CAP, sub, LANES), jnp.int16),
        ),
        in_specs=[hbm] * 5,
        out_specs=(hbm, hbm, hbm),
        scratch_shapes=[
            pltpu.VMEM((n, LANES), jnp.int32),
            pltpu.VMEM((1, tiles), jnp.int32),
            pltpu.VMEM((1, tiles), jnp.int32),
            pltpu.VMEM(background.shape, jnp.bfloat16),
            pltpu.VMEM((n, LANES), jnp.float32),
            pltpu.VMEM(image2.shape, jnp.float32),
            pltpu.VMEM((planes * per_owner, sub, LANES), jnp.bfloat16),
            pltpu.VMEM(system_blocks.shape, jnp.bfloat16),
            pltpu.VMEM((n, LANES), jnp.int32),
            pltpu.VMEM((8, LANES), jnp.int32),
            pltpu.SMEM((n, LANES), jnp.int32),
            pltpu.SMEM((8, LANES), jnp.int32),
            pltpu.SMEM((n, LANES), jnp.int32),
            pltpu.VMEM((n * CAP, sub, LANES), jnp.bfloat16),
            pltpu.VMEM((n * CAP, sub, LANES), jnp.bfloat16),
            pltpu.VMEM((tiles, sub, LANES), jnp.float32),
            pltpu.VMEM((tiles, sub, LANES), jnp.int16),
            pltpu.VMEM((n * CAP, sub, LANES), jnp.int16),
            pltpu.SemaphoreType.DMA((7,)),
            pltpu.SemaphoreType.DMA((2,)),
            pltpu.SemaphoreType.DMA((2,)),
            pltpu.SemaphoreType.DMA((2,)),
            pltpu.SemaphoreType.DMA((2,)),
        ],
        compiler_params=pltpu.CompilerParams(
            collective_id=0, has_side_effects=True, vmem_limit_bytes=67043328
        ),
    )(tile_slab.reshape(1, tiles), tile_block.reshape(1, tiles), image2, system_blocks, background)
    updated = pl.pallas_call(
        functools.partial(update_kernel, (n, tiles, block_rows)),
        out_shape=jax.ShapeDtypeStruct(image2.shape, jnp.float32),
        in_specs=[hbm] * 5,
        out_specs=hbm,
        scratch_shapes=[
            pltpu.SMEM(asked.shape, jnp.int32),
            pltpu.SMEM(scale.shape, jnp.float32),
            pltpu.VMEM(back.shape, back.dtype),
            pltpu.VMEM(image2.shape, jnp.float32),
            pltpu.VMEM(image2.shape, jnp.float32),
            pltpu.VMEM(image2.shape, jnp.float32),
            pltpu.VMEM((planes * per_owner, sub, LANES), jnp.float32),
            pltpu.SemaphoreType.DMA((5,)),
            pltpu.SemaphoreType.DMA((4,)),
        ],
        compiler_params=pltpu.CompilerParams(vmem_limit_bytes=67043328),
    )(asked, scale, back, image2, sens2)
    return updated.reshape(image.shape)


def solution(mesh):
    return jax.shard_map(
        local,
        mesh=mesh,
        in_specs=(
            P("slab", "rep", None),
            P("slab", "rep", None),
            P(("slab", "rep"), None, None),
            P(("slab", "rep"), None),
            P(("slab", "rep")),
            P(("slab", "rep"), None),
        ),
        out_specs=P("slab", "rep", None),
        check_vma=False,
    )
```
